32 devices in a mesh: dp: 1 (over z), sw: 4 (over y), sh: 8 (over x, core).
Axes of the slice: x: 4, y: 4, z: 1, core: 2. Of those that a mesh axis runs over, the one named last changes fastest.
The devices are a block of a 4x4x8 slice.
Arguments:
- features: bfloat16 [1, 512, 6, 96, 24], P('dp', None, None, 'sh', 'sw')
- latent: bfloat16 [1, 16, 6, 96, 24], P('dp', None, None, 'sh', 'sw')
- gn_gain: float32 [2, 2, 512], replicated
- gn_bias: float32 [2, 2, 512], replicated
- zy_weight: bfloat16 [2, 2, 16, 512], replicated
- zy_bias: float32 [2, 2, 512], replicated
- zb_weight: bfloat16 [2, 2, 16, 512], replicated
- zb_bias: float32 [2, 2, 512], replicated
- conv_weight: bfloat16 [2, 2, 512, 512, 3, 3, 3], replicated
- conv_bias: float32 [2, 2, 512], replicated
- up_weight: bfloat16 [512, 512, 3, 3], replicated
- up_bias: float32 [512], replicated
Outputs:
- output: bfloat16 [1, 512, 6, 192, 48], P('dp', None, None, 'sh', 'sw')
All inputs are finite; a program needn't handle non-finite values.
Results may differ from the reference program's by a relative error of at most 0.0137178.
Values are sent between devices in bfloat16 or wider.
A program may use at most 768 MiB of HBM per device.

```python
import jax
import jax.numpy as jnp
from jax import lax

CHANNELS = 512
LATENT = 16
GROUPS = 32
RES_BLOCKS = 2
FRAMES = 6
HEIGHT = 96
WIDTH = 24
GN_EPSILON = 1e-6
CONV_DIMS = ("NCDHW", "OIDHW", "NCDHW")


def setup_inputs(seed: int = 0, part: int = 0) -> dict:
    part_key = jax.random.fold_in(jax.random.key(seed), part)
    data_keys = jax.random.split(part_key, 6)
    weight_keys = jax.random.split(jax.random.key(seed + 1), 10)
    ramp_h = jnp.linspace(-1.0, 1.0, HEIGHT)[:, None]
    ramp_w = jnp.linspace(-1.0, 1.0, WIDTH)[None, :]
    amp_rows = jax.random.normal(data_keys[0], (CHANNELS, 1, 1, 1), jnp.float32)
    amp_cols = jax.random.normal(data_keys[1], (CHANNELS, 1, 1, 1), jnp.float32)
    noise = jax.random.normal(data_keys[2], (CHANNELS, FRAMES, HEIGHT, WIDTH), jnp.float32)
    features = (noise + amp_rows * ramp_h + amp_cols * ramp_w)[None].astype(jnp.bfloat16)
    lat_rows = jax.random.normal(data_keys[3], (LATENT, 1, 1, 1), jnp.float32)
    lat_cols = jax.random.normal(data_keys[4], (LATENT, 1, 1, 1), jnp.float32)
    lat_noise = jax.random.normal(data_keys[5], (LATENT, FRAMES, HEIGHT, WIDTH), jnp.float32)
    latent = (lat_noise + lat_rows * ramp_h + lat_cols * ramp_w)[None].astype(jnp.bfloat16)
    vec_shape = (RES_BLOCKS, 2, CHANNELS)
    map_shape = (RES_BLOCKS, 2, LATENT, CHANNELS)
    gn_gain = 1.0 + 0.3 * jax.random.normal(weight_keys[0], vec_shape, jnp.float32)
    gn_bias = 0.3 * jax.random.normal(weight_keys[1], vec_shape, jnp.float32)
    zy_weight = (jax.random.normal(weight_keys[2], map_shape, jnp.float32) * (0.5 * LATENT ** -0.5)).astype(jnp.bfloat16)
    zy_bias = 1.0 + 0.3 * jax.random.normal(weight_keys[3], vec_shape, jnp.float32)
    zb_weight = (jax.random.normal(weight_keys[4], map_shape, jnp.float32) * (0.5 * LATENT ** -0.5)).astype(jnp.bfloat16)
    zb_bias = 0.3 * jax.random.normal(weight_keys[5], vec_shape, jnp.float32)
    conv_weight = (jax.random.normal(weight_keys[6], (RES_BLOCKS, 2, CHANNELS, CHANNELS, 3, 3, 3), jnp.float32) * (27 * CHANNELS) ** -0.5).astype(jnp.bfloat16)
    conv_bias = 0.3 * jax.random.normal(weight_keys[7], vec_shape, jnp.float32)
    up_weight = (jax.random.normal(weight_keys[8], (CHANNELS, CHANNELS, 3, 3), jnp.float32) * (9 * CHANNELS) ** -0.5).astype(jnp.bfloat16)
    up_bias = 0.3 * jax.random.normal(weight_keys[9], (CHANNELS,), jnp.float32)
    return {"features": features, "latent": latent, "gn_gain": gn_gain, "gn_bias": gn_bias, "zy_weight": zy_weight, "zy_bias": zy_bias, "zb_weight": zb_weight, "zb_bias": zb_bias, "conv_weight": conv_weight, "conv_bias": conv_bias, "up_weight": up_weight, "up_bias": up_bias}


def per_channel(values):
    return values[None, :, None, None, None]


def group_norm(values, gain, shift):
    grouped = values.astype(jnp.float32).reshape(1, GROUPS, CHANNELS // GROUPS, FRAMES, HEIGHT, WIDTH)
    group_mean = jnp.mean(grouped, axis=(2, 3, 4, 5), keepdims=True)
    group_var = jnp.mean(jnp.square(grouped - group_mean), axis=(2, 3, 4, 5), keepdims=True)
    normed = ((grouped - group_mean) * lax.rsqrt(group_var + GN_EPSILON)).reshape(1, CHANNELS, FRAMES, HEIGHT, WIDTH)
    return normed * per_channel(gain) + per_channel(shift)


def latent_map(latent, weight, bias):
    return jnp.einsum("nzthw,zc->ncthw", latent.astype(jnp.float32), weight.astype(jnp.float32)) + per_channel(bias)


def causal_conv(activated, weight, bias):
    first_frame = activated[:, :, :1]
    padded = jnp.concatenate([first_frame, first_frame, activated], axis=2)
    padded = jnp.pad(padded, ((0, 0), (0, 0), (0, 0), (1, 1), (1, 1)))
    conv_out = lax.conv_general_dilated(padded.astype(jnp.float32), weight.astype(jnp.float32), (1, 1, 1), "VALID", dimension_numbers=CONV_DIMS)
    return (conv_out + per_channel(bias)).astype(jnp.bfloat16)


def reference(features, latent, gn_gain, gn_bias, zy_weight, zy_bias, zb_weight, zb_bias, conv_weight, conv_bias, up_weight, up_bias):
    hidden = features
    for block in range(RES_BLOCKS):
        branch = hidden
        for slot in range(2):
            normed = group_norm(branch, gn_gain[block, slot], gn_bias[block, slot])
            mixed = normed * latent_map(latent, zy_weight[block, slot], zy_bias[block, slot]) + latent_map(latent, zb_weight[block, slot], zb_bias[block, slot])
            activated = jax.nn.silu(mixed).astype(jnp.bfloat16)
            branch = causal_conv(activated, conv_weight[block, slot], conv_bias[block, slot])
        hidden = (hidden.astype(jnp.float32) + branch.astype(jnp.float32)).astype(jnp.bfloat16)
    upsampled = jnp.repeat(jnp.repeat(hidden, 2, axis=3), 2, axis=4)
    padded = jnp.pad(upsampled, ((0, 0), (0, 0), (0, 0), (1, 1), (1, 1)))
    conv_out = lax.conv_general_dilated(padded.astype(jnp.float32), up_weight[:, :, None].astype(jnp.float32), (1, 1, 1), "VALID", dimension_numbers=CONV_DIMS)
    return (conv_out + per_channel(up_bias)).astype(jnp.bfloat16)
```

```python
import functools

import jax
import jax.numpy as jnp
from jax import lax
from jax.experimental import pallas as pl
from jax.experimental.pallas import tpu as pltpu
from jax.sharding import PartitionSpec as P

NUM_GROUPS = 32
GN_EPSILON = 1e-6
LANES = 128
SLOTS = 8
RING = 4
MESH = pl.DeviceIdType.MESH
F32 = jnp.float32
BF16 = jnp.bfloat16


def limbs(values):
    high = values.astype(BF16)
    rest = values - high.astype(F32)
    mid = rest.astype(BF16)
    low = (rest - mid.astype(F32)).astype(BF16)
    n = values.shape[0]
    pad = jnp.zeros((16 - 3 * n, values.shape[1]), F32)
    return jnp.concatenate([high.astype(F32), mid.astype(F32), low.astype(F32), pad], axis=0).astype(BF16)


def contract_lanes(a, b):
    return lax.dot_general(a, b, (((1,), (1,)), ((), ())), preferred_element_type=F32)


def block_kernel(dims, x_ref, z_ref, gain_ref, shift_ref, zyw_ref, zyb_ref, zbw_ref, zbb_ref, cw_ref, cb_ref, uw_ref, ub_ref, y_ref,
                 ex, colx, cols, zx, zcolx, zcols, zext, stat_all, group, wyb, yb, xk, acc, hidden, wbuf, prod, xu,
                 wsem, hsend, hrecv, zsend, zrecv, ssend, srecv):
    n_sh, n_sw, n_frame, n_row, n_col, n_chan, n_conv = dims
    main = n_col * SLOTS
    wide = (n_col + 2) * SLOTS
    n_dev = n_sh * n_sw
    count = (n_chan // NUM_GROUPS) * n_frame * n_row * n_col * n_dev
    sh = lax.axis_index("sh")
    sw = lax.axis_index("sw")
    me = sw * n_sh + sh
    up, down = (sh + n_sh - 1) % n_sh, (sh + 1) % n_sh
    left, right = (sw + n_sw - 1) % n_sw, (sw + 1) % n_sw

    def weight_start(q):
        slot = q % RING
        for tap in range(9):
            dst = wbuf.at[slot, :, pl.ds(tap * n_chan, n_chan)]

            @pl.when(q < 3 * n_conv)
            def _():
                pltpu.make_async_copy(cw_ref.at[jnp.minimum(q, 3 * n_conv - 1), tap], dst, wsem.at[slot]).start()

            @pl.when(q == 3 * n_conv)
            def _():
                pltpu.make_async_copy(uw_ref.at[tap], dst, wsem.at[slot]).start()

    def weight_wait(q):
        slot = q % RING
        pltpu.make_async_copy(wbuf.at[slot], wbuf.at[slot], wsem.at[slot]).wait()

    for q in range(RING):
        weight_start(jnp.int32(q))

    barrier = pltpu.get_barrier_semaphore()

    def peer_of(k):
        target = (me + k) % n_dev
        return {"sh": target % n_sh, "sw": target // n_sh}

    @pl.loop(1, n_dev)
    def _(k):
        pl.semaphore_signal(barrier, inc=1, device_id=peer_of(k), device_id_type=MESH)

    def halo_copies(rows, recv_cols, send_cols, send_sem, recv_sem):
        table = [
            (rows.at[1], rows.at[n_row + 1], {"sh": up}),
            (rows.at[n_row], rows.at[0], {"sh": down}),
            (send_cols.at[0], recv_cols.at[1, pl.ds(1, n_row)], {"sw": left}),
            (send_cols.at[1], recv_cols.at[0, pl.ds(1, n_row)], {"sw": right}),
            (send_cols.at[0, 0], recv_cols.at[1, n_row + 1], {"sh": up, "sw": left}),
            (send_cols.at[1, 0], recv_cols.at[0, n_row + 1], {"sh": up, "sw": right}),
            (send_cols.at[0, n_row - 1], recv_cols.at[1, 0], {"sh": down, "sw": left}),
            (send_cols.at[1, n_row - 1], recv_cols.at[0, 0], {"sh": down, "sw": right}),
        ]
        return [pltpu.make_async_remote_copy(src_ref=src, dst_ref=dst, send_sem=send_sem.at[k], recv_sem=recv_sem.at[k],
                                             device_id=where, device_id_type=MESH) for k, (src, dst, where) in enumerate(table)]

    def block_halo(par):
        return halo_copies(ex.at[par], colx.at[par], cols.at[par], hsend.at[par], hrecv.at[par])

    def stats_send(par, sums):
        parts = jnp.dot(limbs(sums), group[...], preferred_element_type=F32)
        mine = parts[0:2] + parts[2:4] + parts[4:6]
        stat_all[par, me] = jnp.concatenate([mine, jnp.zeros((6, LANES), F32)], axis=0)

        @pl.loop(1, n_dev)
        def _(k):
            pltpu.make_async_remote_copy(src_ref=stat_all.at[par, me], dst_ref=stat_all.at[par, me], send_sem=ssend.at[par],
                                         recv_sem=srecv.at[par], device_id=peer_of(k), device_id_type=MESH).start()

    def stats_wait(par):
        several = stat_all.at[par, pl.ds(0, n_dev - 1)]
        pltpu.make_async_copy(several, several, srecv.at[par]).wait()
        pltpu.make_async_copy(several, several, ssend.at[par]).wait()

    chan = lax.broadcasted_iota(jnp.int32, (n_chan, LANES), 0)
    first = lax.broadcasted_iota(jnp.int32, (n_chan, LANES), 1) * (n_chan // NUM_GROUPS)
    member = (chan >= first) & (chan < first + n_chan // NUM_GROUPS)
    group[...] = jnp.where(member, 1.0, 0.0).astype(BF16)
    wyb[...] = jnp.zeros_like(wyb)

    def tile_sums(values):
        total = values[0:SLOTS]
        for c in range(1, n_col):
            total = total + values[c * SLOTS:(c + 1) * SLOTS]
        return total

    def sums_of(first_sum, second_sum):
        return jnp.concatenate([jnp.sum(first_sum, axis=0, keepdims=True), jnp.sum(second_sum, axis=0, keepdims=True)], axis=0)

    zero_sums = (jnp.zeros((SLOTS, n_chan), F32), jnp.zeros((SLOTS, n_chan), F32))

    def load_row(r, carry):
        raw = x_ref[r]
        values = raw.astype(F32)
        ex[0, r + 1] = raw
        hidden[r] = raw
        cols[0, 0, r] = values[0:SLOTS].astype(BF16)
        cols[0, 1, r] = values[main - SLOTS:main].astype(BF16)
        latent = z_ref[r]
        wide_latent = latent.astype(F32)
        zx[r + 1] = latent
        zcols[0, r] = wide_latent[0:SLOTS].astype(BF16)
        zcols[1, r] = wide_latent[main - SLOTS:main].astype(BF16)
        return carry[0] + tile_sums(values), carry[1] + tile_sums(values * values)

    start_sums = lax.fori_loop(0, n_row, load_row, zero_sums)

    pl.semaphore_wait(barrier, n_dev - 1)
    for copy in block_halo(0):
        copy.start()
    z_copies = halo_copies(zx, zcolx, zcols, zsend, zrecv)
    for copy in z_copies:
        copy.start()
    stats_send(0, sums_of(*start_sums))
    for copy in z_copies:
        copy.wait()

    @pl.loop(0, n_row + 2)
    def _(r):
        zext[r] = jnp.concatenate([zcolx[0, r].astype(F32), zx[r].astype(F32), zcolx[1, r].astype(F32)], axis=0).astype(BF16)

    row_of = lax.broadcasted_iota(jnp.int32, (wide, n_chan), 0)
    slot_of = lax.broadcasted_iota(jnp.int32, (n_col + 2, SLOTS, n_chan), 1)
    first_valid = jnp.where(sw == 0, SLOTS, 0)
    last_valid = jnp.where(sw == n_sw - 1, wide - SLOTS, wide)

    def inside(r):
        beyond = ((r == 0) & (sh == 0)) | ((r == n_row + 1) & (sh == n_sh - 1))
        end = jnp.where(beyond, 0, last_valid)
        return (row_of >= first_valid) & (row_of < end)

    def wide_row(par, r):
        return jnp.concatenate([colx[par, 0, r].astype(F32), ex[par, r].astype(F32), colx[par, 1, r].astype(F32)], axis=0)

    frame_of = lax.broadcasted_iota(jnp.int32, (n_col, SLOTS, n_chan), 1).reshape(main, n_chan)

    def conv_step(i, _):
        par = i % 2
        after = (i + 1) % 2

        wyb[0:zyw_ref.shape[1], 0:n_chan] = zyw_ref[i]
        wyb[0:zyw_ref.shape[1], n_chan:2 * n_chan] = zbw_ref[i]
        maps = jnp.dot(zext[...].reshape((n_row + 2) * wide, LANES), wyb[...], preferred_element_type=F32)
        map_bias = jnp.concatenate([zyb_ref[i], zbb_ref[i]], axis=1)
        yb[...] = (maps + map_bias).reshape(n_row + 2, wide, 2 * n_chan)

        stats_wait(par)
        total = stat_all[par, 0]
        for d in range(1, n_dev):
            total = total + stat_all[par, d]
        group_mean = total[0:1] / count
        group_var = jnp.maximum(total[1:2] / count - group_mean * group_mean, 0.0)
        both = jnp.concatenate([group_mean, lax.rsqrt(group_var + GN_EPSILON)], axis=0)
        spread = contract_lanes(limbs(both), group[...])
        chan_both = spread[0:2] + spread[2:4] + spread[4:6]
        mean = chan_both[0:1]
        scale = chan_both[1:2] * gain_ref[i]
        shift = shift_ref[i]
        for copy in block_halo(par):
            copy.wait()

        @pl.loop(0, n_row + 2)
        def _(r):
            normed = (wide_row(par, r) - mean) * scale + shift
            mixed = normed * yb[r, :, 0:n_chan] + yb[r, :, n_chan:2 * n_chan]
            act = jnp.where(inside(r), mixed * jax.nn.sigmoid(mixed), 0.0)
            taps = act.reshape(n_col + 2, SLOTS, n_chan)
            for kt in (2, 1, 0):
                for dw in range(3):
                    xk[kt, r, :, dw * n_chan:(dw + 1) * n_chan] = taps[dw:dw + n_col].reshape(main, n_chan).astype(BF16)
                if kt > 0:
                    taps = jnp.where(slot_of == 0, taps, pltpu.roll(taps, 1, 1))

        @pl.loop(0, 3)
        def _(kt):
            q = i * 3 + kt
            weight_wait(q)
            lhs = jnp.concatenate([xk[kt, dh:dh + n_row].reshape(n_row * main, 3 * n_chan) for dh in range(3)], axis=1)
            part = contract_lanes(lhs, wbuf[q % RING])

            @pl.when(kt == 0)
            def _():
                acc[...] = part

            @pl.when(kt > 0)
            def _():
                acc[...] = acc[...] + part

            @pl.when(q + RING <= 3 * n_conv)
            def _():
                weight_start(q + RING)

        bias = cb_ref[i]
        second = i % 2 == 1

        def finish_row(r, carry):
            conv = (acc[pl.ds(pl.multiple_of(r * main, main), main), :] + bias).astype(BF16).astype(F32)
            old = hidden[r].astype(F32)
            value = jnp.where(second, old + conv, conv).astype(BF16).astype(F32)
            value = jnp.where(frame_of < n_frame, value, 0.0)
            hidden[r] = jnp.where(second, value, old).astype(BF16)
            ex[after, r + 1] = value.astype(BF16)
            cols[after, 0, r] = value[0:SLOTS].astype(BF16)
            cols[after, 1, r] = value[main - SLOTS:main].astype(BF16)
            return carry[0] + tile_sums(value), carry[1] + tile_sums(value * value)

        sums = lax.fori_loop(0, n_row, finish_row, zero_sums)
        for copy in block_halo(after):
            copy.start()

        @pl.when(i < n_conv - 1)
        def _():
            stats_send(after, sums_of(*sums))

        return 0

    lax.fori_loop(0, n_conv, conv_step, 0)

    par = n_conv % 2
    for copy in block_halo(par):
        copy.wait()

    @pl.loop(0, n_row + 2)
    def _(r):
        xu[r] = jnp.where(inside(r), wide_row(par, r), 0.0).astype(BF16)

    last = 3 * n_conv
    weight_wait(last)

    @pl.loop(0, 3)
    def _(dy):
        begin = jnp.minimum(dy, 1)
        lhs = xu[pl.ds(begin, n_row + 1)].reshape((n_row + 1) * wide, n_chan)
        for dx in range(3):
            w = wbuf[last % RING, :, pl.ds(pl.multiple_of((dy * 3 + dx) * n_chan, n_chan), n_chan)]
            prod[dy, :, :, dx * n_chan:(dx + 1) * n_chan] = contract_lanes(lhs, w).reshape(n_row + 1, wide, n_chan)

    up_bias = ub_ref[...]

    @pl.loop(0, n_row)
    def _(r):
        for py in range(2):
            def of(dx, lo):
                at = (slice(lo, lo + main), slice(dx * n_chan, (dx + 1) * n_chan))
                return prod[(0, r + py) + at] + prod[(1, r) + at] + prod[(2, r + py) + at]

            middle = of(1, SLOTS) + up_bias
            phases = [of(0, 0) + middle + of(2, SLOTS), of(0, SLOTS) + middle + of(2, 2 * SLOTS)]
            tiles = [phases[px][c * SLOTS:(c + 1) * SLOTS] for c in range(n_col) for px in range(2)]
            y_ref[2 * r + py] = jnp.concatenate(tiles, axis=0).astype(BF16)


def solution(mesh):
    n_sh = mesh.shape["sh"]
    n_sw = mesh.shape["sw"]

    def local_step(features, latent, gn_gain, gn_bias, zy_weight, zy_bias, zb_weight, zb_bias, conv_weight, conv_bias, up_weight, up_bias):
        _, n_chan, n_frame, n_row, n_col = features.shape
        n_latent = latent.shape[1]
        n_conv = gn_gain.shape[0] * gn_gain.shape[1]
        main = n_col * SLOTS
        wide = main + 2 * SLOTS
        n_dev = n_sh * n_sw

        def tiles_of(values, lanes):
            moved = jnp.transpose(values[0], (2, 3, 1, 0))
            padded = jnp.pad(moved, ((0, 0), (0, 0), (0, SLOTS - n_frame), (0, lanes - values.shape[1])))
            return padded.reshape(n_row, main, lanes)

        vector = lambda values: values.reshape(n_conv, 1, n_chan)
        small = lambda values: values.reshape(n_conv, n_latent, n_chan)
        taps = jnp.transpose(conv_weight, (0, 1, 4, 5, 6, 2, 3)).reshape(3 * n_conv, 9, n_chan, n_chan)
        up_taps = jnp.transpose(up_weight, (2, 3, 0, 1)).reshape(9, n_chan, n_chan)
        dims = (n_sh, n_sw, n_frame, n_row, n_col, n_chan, n_conv)
        vmem = pl.BlockSpec(memory_space=pltpu.VMEM)
        hbm = pl.BlockSpec(memory_space=pl.ANY)
        dma = pltpu.SemaphoreType.DMA
        rows = n_row + 2
        result = pl.pallas_call(
            functools.partial(block_kernel, dims),
            out_shape=jax.ShapeDtypeStruct((2 * n_row, 2 * main, n_chan), BF16),
            in_specs=[vmem] * 8 + [hbm, vmem, hbm, vmem],
            out_specs=vmem,
            scratch_shapes=[
                pltpu.VMEM((2, rows, main, n_chan), BF16),
                pltpu.VMEM((2, 2, rows, SLOTS, n_chan), BF16),
                pltpu.VMEM((2, 2, n_row, SLOTS, n_chan), BF16),
                pltpu.VMEM((rows, main, LANES), BF16),
                pltpu.VMEM((2, rows, SLOTS, LANES), BF16),
                pltpu.VMEM((2, n_row, SLOTS, LANES), BF16),
                pltpu.VMEM((rows, wide, LANES), BF16),
                pltpu.VMEM((2, n_dev, 8, LANES), F32),
                pltpu.VMEM((n_chan, LANES), BF16),
                pltpu.VMEM((LANES, 2 * n_chan), BF16),
                pltpu.VMEM((rows, wide, 2 * n_chan), F32),
                pltpu.VMEM((3, rows, main, 3 * n_chan), BF16),
                pltpu.VMEM((n_row * main, n_chan), F32),
                pltpu.VMEM((n_row, main, n_chan), BF16),
                pltpu.VMEM((RING, n_chan, 9 * n_chan), BF16),
                pltpu.VMEM((3, n_row + 1, wide, 3 * n_chan), F32),
                pltpu.VMEM((rows, wide, n_chan), BF16),
                dma((RING,)),
                dma((2, 8)),
                dma((2, 8)),
                dma((8,)),
                dma((8,)),
                dma((2,)),
                dma((2,)),
            ],
            compiler_params=pltpu.CompilerParams(collective_id=0, has_side_effects=True, vmem_limit_bytes=64 * 1024 * 1024 - 65536 - 4096),
            name="decoder_block",
        )(tiles_of(features, n_chan), tiles_of(latent, LANES), vector(gn_gain), vector(gn_bias), small(zy_weight), vector(zy_bias),
          small(zb_weight), vector(zb_bias), taps, vector(conv_bias), up_taps, up_bias.reshape(1, n_chan))
        frames = result.reshape(2 * n_row, 2 * n_col, SLOTS, n_chan)[:, :, :n_frame]
        return jnp.transpose(frames, (3, 2, 0, 1))[None]

    data_spec = P("dp", None, None, "sh", "sw")
    return jax.shard_map(local_step, mesh=mesh, in_specs=(data_spec, data_spec) + (P(),) * 10, out_specs=data_spec, check_vma=False)
```

```python
import functools

import jax
import jax.numpy as jnp
from jax import lax
from jax.experimental import pallas as pl
from jax.experimental.pallas import tpu as pltpu
from jax.sharding import PartitionSpec as P

NUM_GROUPS = 32
GN_EPSILON = 1e-6
LANES = 128
SLOTS = 8
RING = 9
MESH = pl.DeviceIdType.MESH
F32 = jnp.float32
BF16 = jnp.bfloat16


def limbs(values):
    high = values.astype(BF16)
    rest = values - high.astype(F32)
    mid = rest.astype(BF16)
    low = (rest - mid.astype(F32)).astype(BF16)
    n = values.shape[0]
    pad = jnp.zeros((16 - 3 * n, values.shape[1]), F32)
    return jnp.concatenate([high.astype(F32), mid.astype(F32), low.astype(F32), pad], axis=0).astype(BF16)


def contract_lanes(a, b):
    return lax.dot_general(a, b, (((1,), (1,)), ((), ())), preferred_element_type=F32)


def block_kernel(dims, x_ref, z_ref, gain_ref, shift_ref, zyw_ref, zyb_ref, zbw_ref, zbb_ref, cw_ref, cb_ref, uw_ref, ub_ref, y_ref,
                 ex, colx, cols, zx, zcolx, zcols, zext, stat_all, group, wyb, yb, xk, acc, hidden, wbuf, prod, xt, zt,
                 wsem, hsend, hrecv, zsend, zrecv, ssend, srecv):
    n_sh, n_sw, n_frame, n_row, n_col, n_chan, n_conv = dims
    half = n_chan // 2
    main = n_col * SLOTS
    wide = (n_col + 2) * SLOTS
    n_dev = n_sh * n_sw
    per_group = n_chan // NUM_GROUPS
    count = per_group * n_frame * n_row * n_col * n_dev
    sh = lax.axis_index("sh")
    sw = lax.axis_index("sw")
    me = sw * n_sh + sh
    up, down = (sh + n_sh - 1) % n_sh, (sh + 1) % n_sh
    left, right = (sw + n_sw - 1) % n_sw, (sw + 1) % n_sw

    last_group = 6 * n_conv

    def weight_start(g):
        slot = g % RING
        source = (g // 6) * 3 + g % 3
        from_half = (g // 3) % 2
        for tap in range(9):
            dst = wbuf.at[slot, :, pl.ds(tap * half, half)]

            @pl.when(g < last_group)
            def _():
                lanes = pl.ds(pl.multiple_of(from_half * half, half), half)
                pltpu.make_async_copy(cw_ref.at[jnp.minimum(source, 3 * n_conv - 1), tap, :, lanes], dst, wsem.at[slot]).start()

            @pl.when((g >= last_group) & (g < last_group + 2))
            def _():
                lanes = pl.ds(pl.multiple_of(jnp.clip(g - last_group, 0, 1) * half, half), half)
                pltpu.make_async_copy(uw_ref.at[tap, :, lanes], dst, wsem.at[slot]).start()

    def weight_wait(g):
        slot = g % RING
        pltpu.make_async_copy(wbuf.at[slot], wbuf.at[slot], wsem.at[slot]).wait()

    @pl.loop(0, RING)
    def _(g):
        weight_start(g)

    barrier = pltpu.get_barrier_semaphore()
    peers = [{"sh": (sh + b) % n_sh, "sw": (sw + a) % n_sw} for a in range(n_sw) for b in range(n_sh)][1:]
    for peer in peers:
        pl.semaphore_signal(barrier, inc=1, device_id=peer, device_id_type=MESH)

    def halo_copies(rows, recv_cols, send_cols, send_sem, recv_sem):
        table = [
            (send_cols.at[0], recv_cols.at[1, pl.ds(1, n_row)], {"sw": left}),
            (send_cols.at[1], recv_cols.at[0, pl.ds(1, n_row)], {"sw": right}),
            (rows.at[1], rows.at[n_row + 1], {"sh": up}),
            (rows.at[n_row], rows.at[0], {"sh": down}),
            (send_cols.at[0, 0], recv_cols.at[1, n_row + 1], {"sh": up, "sw": left}),
            (send_cols.at[1, 0], recv_cols.at[0, n_row + 1], {"sh": up, "sw": right}),
            (send_cols.at[0, n_row - 1], recv_cols.at[1, 0], {"sh": down, "sw": left}),
            (send_cols.at[1, n_row - 1], recv_cols.at[0, 0], {"sh": down, "sw": right}),
        ]
        return [pltpu.make_async_remote_copy(src_ref=src, dst_ref=dst, send_sem=send_sem.at[k], recv_sem=recv_sem.at[k],
                                             device_id=where, device_id_type=MESH) for k, (src, dst, where) in enumerate(table)]

    def block_halo(par, h):
        return halo_copies(ex.at[par, h], colx.at[par, h], cols.at[par, h], hsend.at[par, h], hrecv.at[par, h])

    def stats_send(par, h, first_sum, second_sum):
        both = jnp.concatenate([jnp.sum(first_sum, axis=0, keepdims=True), jnp.sum(second_sum, axis=0, keepdims=True)], axis=1)
        parts = jnp.dot(limbs(both), group[...], preferred_element_type=F32)
        stat_all[par, h, me] = parts[0:1] + parts[1:2] + parts[2:3]
        for peer in peers:
            pltpu.make_async_remote_copy(src_ref=stat_all.at[par, h, me], dst_ref=stat_all.at[par, h, me], send_sem=ssend.at[par, h],
                                         recv_sem=srecv.at[par, h], device_id=peer, device_id_type=MESH).start()

    def stats_wait(par, h):
        several = stat_all.at[par, h, pl.ds(0, n_dev - 1)]
        pltpu.make_async_copy(several, several, srecv.at[par, h]).wait()
        pltpu.make_async_copy(several, several, ssend.at[par, h]).wait()

    def vector(ref, i, h):
        return ref[i // 2, pl.ds(i % 2, 1), h * half:(h + 1) * half]

    chan = lax.broadcasted_iota(jnp.int32, (2 * half, LANES), 0)
    lane = lax.broadcasted_iota(jnp.int32, (2 * half, LANES), 1)
    first = jnp.where(lane < LANES // 2, lane * per_group, (lane - LANES // 2) * per_group + half)
    limit = jnp.where(lane < LANES // 2, half, 2 * half)
    member = (chan >= first) & (chan < first + per_group) & (first < limit)
    group[...] = jnp.where(member, 1.0, 0.0).astype(BF16)
    wyb[...] = jnp.zeros_like(wyb)
    xt[...] = jnp.zeros_like(xt)
    zt[...] = jnp.zeros_like(zt)

    def tile_sums(values):
        total = values[0:SLOTS]
        for c in range(1, n_col):
            total = total + values[c * SLOTS:(c + 1) * SLOTS]
        return total

    def no_sums(width):
        return jnp.zeros((SLOTS, width), F32), jnp.zeros((SLOTS, width), F32)

    def load_row(r, carry):
        for f in range(n_frame):
            moved = x_ref[f, r].astype(F32)
            for k in range(n_chan // LANES):
                xt[k, pl.ds(f, n_col, stride=SLOTS), :] = moved[:, k * LANES:(k + 1) * LANES]
        values = jnp.concatenate([xt[k] for k in range(n_chan // LANES)], axis=1)
        hidden[r] = values.astype(BF16)
        for h in range(2):
            part = values[:, h * half:(h + 1) * half]
            ex[0, h, r + 1] = part.astype(BF16)
            cols[0, h, 0, r] = part[0:SLOTS].astype(BF16)
            cols[0, h, 1, r] = part[main - SLOTS:main].astype(BF16)
        for c in range(n_col):
            zt[c * SLOTS:c * SLOTS + n_frame, 0:z_ref.shape[3]] = z_ref[r, c].astype(F32)
        latent = zt[...]
        zx[r + 1] = latent.astype(BF16)
        zcols[0, r] = latent[0:SLOTS].astype(BF16)
        zcols[1, r] = latent[main - SLOTS:main].astype(BF16)
        return carry[0] + tile_sums(values), carry[1] + tile_sums(values * values)

    start_sums = lax.fori_loop(0, n_row, load_row, no_sums(n_chan))

    pl.semaphore_wait(barrier, n_dev - 1)
    z_copies = halo_copies(zx, zcolx, zcols, zsend, zrecv)
    for h in range(2):
        stats_send(0, h, start_sums[0][:, h * half:(h + 1) * half], start_sums[1][:, h * half:(h + 1) * half])
        if h == 0:
            for copy in z_copies:
                copy.start()
        for copy in block_halo(0, h):
            copy.start()
    for copy in z_copies:
        copy.wait()

    @pl.loop(0, n_row + 2)
    def _(r):
        zext[r] = jnp.concatenate([zcolx[0, r].astype(F32), zx[r].astype(F32), zcolx[1, r].astype(F32)], axis=0).astype(BF16)

    row_of = lax.broadcasted_iota(jnp.int32, (wide, half), 0)
    slot_of = lax.broadcasted_iota(jnp.int32, (n_col + 2, SLOTS, half), 1)
    first_valid = jnp.where(sw == 0, SLOTS, 0)
    last_valid = jnp.where(sw == n_sw - 1, wide - SLOTS, wide)

    def inside(r):
        beyond = ((r == 0) & (sh == 0)) | ((r == n_row + 1) & (sh == n_sh - 1))
        end = jnp.where(beyond, 0, last_valid)
        return (row_of >= first_valid) & (row_of < end)

    def wide_row(par, h, r):
        return jnp.concatenate([colx[par, h, 0, r].astype(F32), ex[par, h, r].astype(F32), colx[par, h, 1, r].astype(F32)], axis=0)

    frame_of = lax.broadcasted_iota(jnp.int32, (n_col, SLOTS, half), 1).reshape(main, half)

    def activate(i, par, h):
        stats_wait(par, h)
        total = stat_all[par, h, 0]
        for d in range(1, n_dev):
            total = total + stat_all[par, h, d]
        total = total / count
        group_var = jnp.maximum(pltpu.roll(total, LANES // 2, 1) - total * total, 0.0)
        parts = contract_lanes(limbs(jnp.concatenate([total, lax.rsqrt(group_var + GN_EPSILON)], axis=0)), group[0:half])
        chan_both = parts[0:2] + parts[2:4] + parts[4:6]
        mean = chan_both[0:1]
        scale = chan_both[1:2] * vector(gain_ref, i, h)
        shift = vector(shift_ref, i, h)
        for copy in block_halo(par, h):
            copy.wait()

        @pl.loop(0, n_row + 2)
        def _(r):
            normed = (wide_row(par, h, r) - mean) * scale + shift
            mixed = normed * yb[r, :, h * half:(h + 1) * half] + yb[r, :, n_chan + h * half:n_chan + (h + 1) * half]
            act = jnp.where(inside(r), mixed * jax.nn.sigmoid(mixed), 0.0)
            taps = act.reshape(n_col + 2, SLOTS, half)
            for kt in (2, 1, 0):
                for dw in range(3):
                    xk[h, kt, r, :, dw * half:(dw + 1) * half] = taps[dw:dw + n_col].reshape(main, half).astype(BF16)
                if kt > 0:
                    taps = jnp.where(slot_of == 0, taps, pltpu.roll(taps, 1, 1))

    def taps_of(h):
        return jnp.concatenate([xk[h, kt, dh:dh + n_row].reshape(n_row * main, 3 * half) for kt in range(3) for dh in range(3)], axis=1)

    def release(g):
        @pl.loop(g, g + 3)
        def _(k):
            weight_start(k + RING)

    def conv_step(i, _):
        par = i % 2
        after = (i + 1) % 2
        g = 6 * i

        wyb[0:zyw_ref.shape[1], 0:n_chan] = zyw_ref[i]
        wyb[0:zyw_ref.shape[1], n_chan:2 * n_chan] = zbw_ref[i]
        maps = jnp.dot(zext[...].reshape((n_row + 2) * wide, LANES), wyb[...], preferred_element_type=F32)
        map_bias = jnp.concatenate([vector(ref, i, h) for ref in (zyb_ref, zbb_ref) for h in range(2)], axis=1)
        yb[...] = (maps + map_bias).reshape(n_row + 2, wide, 2 * n_chan)

        activate(i, par, 0)
        for kt in range(3):
            weight_wait(g + kt)
        acc[...] = contract_lanes(taps_of(0), jnp.concatenate([wbuf[(g + kt) % RING] for kt in range(3)], axis=1))
        release(g)
        activate(i, par, 1)
        for kt in range(3):
            weight_wait(g + 3 + kt)

        second = i % 2 == 1

        def out_half(o, _):
            chans = pl.ds(pl.multiple_of(o * half, half), half)
            w = jnp.concatenate([wbuf[(g + 3 + kt) % RING, chans, :] for kt in range(3)], axis=1)
            acc[:, chans] = acc[:, chans] + contract_lanes(taps_of(1), w)
            bias = cb_ref[i // 2, pl.ds(i % 2, 1), chans]

            def finish_row(r, carry):
                conv = (acc[pl.ds(pl.multiple_of(r * main, main), main), chans] + bias).astype(BF16).astype(F32)
                old = hidden[r, :, chans].astype(F32)
                value = jnp.where(second, old + conv, conv).astype(BF16).astype(F32)
                value = jnp.where(frame_of < n_frame, value, 0.0)
                hidden[r, :, chans] = jnp.where(second, value, old).astype(BF16)
                ex[after, o, r + 1] = value.astype(BF16)
                cols[after, o, 0, r] = value[0:SLOTS].astype(BF16)
                cols[after, o, 1, r] = value[main - SLOTS:main].astype(BF16)
                return carry[0] + tile_sums(value), carry[1] + tile_sums(value * value)

            sums = lax.fori_loop(0, n_row, finish_row, no_sums(half))

            @pl.when(i < n_conv - 1)
            def _():
                stats_send(after, o, *sums)

            for copy in block_halo(after, o):
                copy.start()
            return 0

        lax.fori_loop(0, 2, out_half, 0)
        release(g + 3)
        return 0

    lax.fori_loop(0, n_conv, conv_step, 0)

    par = n_conv % 2

    def edges(h):
        for copy in block_halo(par, h):
            copy.wait()

        @pl.loop(0, n_row + 2)
        def _(r):
            value = jnp.where(inside(r), wide_row(par, h, r), 0.0).astype(BF16)
            xk[h, 0, r, :, 0:half] = value[0:main]
            xk[h, 1, r, 0:2 * SLOTS, 0:half] = value[main:wide]

    def products(h, dy):
        begin = jnp.minimum(dy, 1)
        rows = pl.ds(begin, n_row + 1)
        lhs = jnp.concatenate([xk[h, 0, rows, :, 0:half], xk[h, 1, rows, 0:2 * SLOTS, 0:half]], axis=1)
        lhs = lhs.reshape((n_row + 1) * wide, half)
        for dx in range(3):
            w = wbuf[(last_group + h) % RING, :, pl.ds(pl.multiple_of((dy * 3 + dx) * half, half), half)]
            product = contract_lanes(lhs, w).reshape(n_row + 1, wide, n_chan)
            lanes = slice(dx * n_chan, (dx + 1) * n_chan)
            prod[dy, :, :, lanes] = product if h == 0 else prod[dy, :, :, lanes] + product

    for h in range(2):
        edges(h)
        weight_wait(last_group + h)

        @pl.loop(0, 3)
        def _(dy):
            products(h, dy)

    up_bias = ub_ref[...]

    @pl.loop(0, n_row)
    def _(r):
        for py in range(2):
            def of(dx, lo):
                at = (slice(lo, lo + main), slice(dx * n_chan, (dx + 1) * n_chan))
                return prod[(0, r + py) + at] + prod[(1, r) + at] + prod[(2, r + py) + at]

            middle = of(1, SLOTS) + up_bias
            phases = [of(0, 0) + middle + of(2, SLOTS), of(0, SLOTS) + middle + of(2, 2 * SLOTS)]
            tiles = [phases[px][c * SLOTS:(c + 1) * SLOTS] for c in range(n_col) for px in range(2)]
            y_ref[2 * r + py] = jnp.concatenate(tiles, axis=0).astype(BF16)


def solution(mesh):
    n_sh = mesh.shape["sh"]
    n_sw = mesh.shape["sw"]

    def local_step(features, latent, gn_gain, gn_bias, zy_weight, zy_bias, zb_weight, zb_bias, conv_weight, conv_bias, up_weight, up_bias):
        _, n_chan, n_frame, n_row, n_col = features.shape
        n_latent = latent.shape[1]
        n_conv = gn_gain.shape[0] * gn_gain.shape[1]
        main = n_col * SLOTS
        wide = main + 2 * SLOTS
        n_dev = n_sh * n_sw
        half = n_chan // 2

        small = lambda values: values.reshape(n_conv, n_latent, n_chan)
        taps = jnp.transpose(conv_weight, (0, 1, 4, 5, 6, 2, 3)).reshape(3 * n_conv, 9, n_chan, n_chan)
        up_taps = jnp.transpose(up_weight, (2, 3, 0, 1)).reshape(9, n_chan, n_chan)
        dims = (n_sh, n_sw, n_frame, n_row, n_col, n_chan, n_conv)
        vmem = pl.BlockSpec(memory_space=pltpu.VMEM)
        hbm = pl.BlockSpec(memory_space=pl.ANY)
        dma = pltpu.SemaphoreType.DMA
        rows = n_row + 2
        result = pl.pallas_call(
            functools.partial(block_kernel, dims),
            out_shape=jax.ShapeDtypeStruct((2 * n_row, 2 * main, n_chan), BF16),
            in_specs=[vmem] * 8 + [hbm, vmem, hbm, vmem],
            out_specs=vmem,
            scratch_shapes=[
                pltpu.VMEM((2, 2, rows, main, half), BF16),
                pltpu.VMEM((2, 2, 2, rows, SLOTS, half), BF16),
                pltpu.VMEM((2, 2, 2, n_row, SLOTS, half), BF16),
                pltpu.VMEM((rows, main, LANES), BF16),
                pltpu.VMEM((2, rows, SLOTS, LANES), BF16),
                pltpu.VMEM((2, n_row, SLOTS, LANES), BF16),
                pltpu.VMEM((rows, wide, LANES), BF16),
                pltpu.VMEM((2, 2, n_dev, 1, LANES), F32),
                pltpu.VMEM((n_chan, LANES), BF16),
                pltpu.VMEM((LANES, 2 * n_chan), BF16),
                pltpu.VMEM((rows, wide, 2 * n_chan), F32),
                pltpu.VMEM((2, 3, rows, main, 3 * half), BF16),
                pltpu.VMEM((n_row * main, n_chan), F32),
                pltpu.VMEM((n_row, main, n_chan), BF16),
                pltpu.VMEM((RING, n_chan, 9 * half), BF16),
                pltpu.VMEM((3, n_row + 1, wide, 3 * n_chan), F32),
                pltpu.VMEM((n_chan // LANES, main, LANES), F32),
                pltpu.VMEM((main, LANES), F32),
                dma((RING,)),
                dma((2, 2, 8)),
                dma((2, 2, 8)),
                dma((8,)),
                dma((8,)),
                dma((2, 2)),
                dma((2, 2)),
            ],
            compiler_params=pltpu.CompilerParams(collective_id=0, has_side_effects=True, vmem_limit_bytes=64 * 1024 * 1024 - 65536 - 4096),
            name="decoder_block",
        )(jnp.transpose(features[0], (1, 2, 3, 0)), jnp.transpose(latent[0], (2, 3, 1, 0)), gn_gain, gn_bias, small(zy_weight), zy_bias,
          small(zb_weight), zb_bias, taps, conv_bias, up_taps, up_bias.reshape(1, n_chan))
        frames = result.reshape(2 * n_row, 2 * n_col, SLOTS, n_chan)[:, :, :n_frame]
        return jnp.transpose(frames, (3, 2, 0, 1))[None]

    data_spec = P("dp", None, None, "sh", "sw")
    return jax.shard_map(local_step, mesh=mesh, in_specs=(data_spec, data_spec) + (P(),) * 10, out_specs=data_spec, check_vma=False)
```

```python
import functools

import jax
import jax.numpy as jnp
from jax import lax
from jax.experimental import pallas as pl
from jax.experimental.pallas import tpu as pltpu
from jax.sharding import PartitionSpec as P

NUM_GROUPS = 32
GN_EPSILON = 1e-6
LANES = 128
SLOTS = 8
RING = 9
MESH = pl.DeviceIdType.MESH
F32 = jnp.float32
BF16 = jnp.bfloat16


def limbs(values):
    high = values.astype(BF16)
    rest = values - high.astype(F32)
    mid = rest.astype(BF16)
    low = (rest - mid.astype(F32)).astype(BF16)
    n = values.shape[0]
    pad = jnp.zeros((16 - 3 * n, values.shape[1]), F32)
    return jnp.concatenate([high.astype(F32), mid.astype(F32), low.astype(F32), pad], axis=0).astype(BF16)


def contract_lanes(a, b):
    return lax.dot_general(a, b, (((1,), (1,)), ((), ())), preferred_element_type=F32)


def block_kernel(dims, x_ref, z_ref, gain_ref, shift_ref, zyw_ref, zyb_ref, zbw_ref, zbb_ref, cw_ref, cb_ref, uw_ref, ub_ref, y_ref,
                 ex, colx, cols, zx, zcolx, zcols, zext, stat_all, group, wyb, yb, xk, acc, hidden, wbuf, prod, xt, zt,
                 wsem, hsend, hrecv, zsend, zrecv, ssend, srecv):
    n_sh, n_sw, n_frame, n_row, n_col, n_chan, n_conv = dims
    half = n_chan // 2
    main = n_col * SLOTS
    wide = (n_col + 2) * SLOTS
    n_dev = n_sh * n_sw
    per_group = n_chan // NUM_GROUPS
    count = per_group * n_frame * n_row * n_col * n_dev
    sh = lax.axis_index("sh")
    sw = lax.axis_index("sw")
    me = sw * n_sh + sh
    up, down = (sh + n_sh - 1) % n_sh, (sh + 1) % n_sh
    left, right = (sw + n_sw - 1) % n_sw, (sw + 1) % n_sw

    barrier = pltpu.get_barrier_semaphore()
    hops = lambda a, b: min(a, n_sw - a) + min(b, n_sh - b) / 2
    offsets = sorted(((a, b) for a in range(n_sw) for b in range(n_sh)), key=lambda ab: -hops(*ab))[:-1]
    rows_of, cols_of = [(sh + b) % n_sh for b in range(n_sh)], [(sw + a) % n_sw for a in range(n_sw)]
    peers = [{"sh": rows_of[b], "sw": cols_of[a]} for a, b in offsets]
    for peer in peers:
        pl.semaphore_signal(barrier, inc=1, device_id=peer, device_id_type=MESH)

    last_group = 6 * n_conv

    def conv_weights(i, h):
        for kt in range(3):
            slot = (6 * i + 3 * h + kt) % RING
            pltpu.make_async_copy(cw_ref.at[3 * i + kt, :, :, pl.ds(h * half, half)], wbuf.at[slot], wsem.at[slot]).start()

    def up_weights():
        for h in range(2):
            slot = (last_group + h) % RING
            pltpu.make_async_copy(uw_ref.at[:, :, pl.ds(h * half, half)], wbuf.at[slot], wsem.at[slot]).start()

    def weight_wait(g):
        slot = g % RING
        pltpu.make_async_copy(wbuf.at[slot], wbuf.at[slot], wsem.at[slot]).wait()

    conv_weights(0, 0)
    conv_weights(0, 1)
    conv_weights(1, 0)

    def halo_copies(rows, recv_cols, send_cols, send_sem, recv_sem):
        table = [
            (send_cols.at[0], recv_cols.at[1, pl.ds(1, n_row)], {"sw": left}),
            (send_cols.at[1], recv_cols.at[0, pl.ds(1, n_row)], {"sw": right}),
            (rows.at[1], rows.at[n_row + 1], {"sh": up}),
            (rows.at[n_row], rows.at[0], {"sh": down}),
            (send_cols.at[0, 0], recv_cols.at[1, n_row + 1], {"sh": up, "sw": left}),
            (send_cols.at[1, 0], recv_cols.at[0, n_row + 1], {"sh": up, "sw": right}),
            (send_cols.at[0, n_row - 1], recv_cols.at[1, 0], {"sh": down, "sw": left}),
            (send_cols.at[1, n_row - 1], recv_cols.at[0, 0], {"sh": down, "sw": right}),
        ]
        return [pltpu.make_async_remote_copy(src_ref=src, dst_ref=dst, send_sem=send_sem.at[k], recv_sem=recv_sem.at[k],
                                             device_id=where, device_id_type=MESH) for k, (src, dst, where) in enumerate(table)]

    def block_halo(par, h):
        return halo_copies(ex.at[par, h], colx.at[par, h], cols.at[par, h], hsend.at[par, h], hrecv.at[par, h])

    def group_row(h, first_sum, second_sum):
        both = jnp.concatenate([jnp.sum(first_sum, axis=0, keepdims=True), jnp.sum(second_sum, axis=0, keepdims=True)], axis=1)
        parts = jnp.dot(limbs(both), group[h], preferred_element_type=F32)
        return parts[0:1] + parts[1:2] + parts[2:3]

    def stats_send(par, h, row):
        stat_all[par, h, me] = row
        for peer in peers:
            pltpu.make_async_remote_copy(src_ref=stat_all.at[par, h, me], dst_ref=stat_all.at[par, h, me], send_sem=ssend.at[par, h],
                                         recv_sem=srecv.at[par, h], device_id=peer, device_id_type=MESH).start()

    def stats_wait(par, h):
        several = stat_all.at[par, h, pl.ds(0, n_dev - 1)]
        pltpu.make_async_copy(several, several, srecv.at[par, h]).wait()
        pltpu.make_async_copy(several, several, ssend.at[par, h]).wait()

    def vector(ref, i, h):
        return ref[i // 2, pl.ds(i % 2, 1), h * half:(h + 1) * half]

    chan = lax.broadcasted_iota(jnp.int32, (2 * half, LANES), 0)
    lane = lax.broadcasted_iota(jnp.int32, (2 * half, LANES), 1)
    squares = lane >= LANES // 2
    for h in range(2):
        first = jnp.where(squares, lane - LANES // 2, lane) * per_group - h * half
        held = (first >= 0) & (first < half)
        first = first + jnp.where(squares, half, 0)
        group[h] = jnp.where(held & (chan >= first) & (chan < first + per_group), 1.0, 0.0).astype(BF16)
    wyb[...] = jnp.zeros_like(wyb)
    xt[...] = jnp.zeros_like(xt)
    zt[...] = jnp.zeros_like(zt)

    def tile_sums(values):
        total = values[0:SLOTS]
        for c in range(1, n_col):
            total = total + values[c * SLOTS:(c + 1) * SLOTS]
        return total

    def no_sums(width):
        return jnp.zeros((SLOTS, width), F32), jnp.zeros((SLOTS, width), F32)

    def load_row(r, carry):
        for f in range(n_frame):
            moved = x_ref[f, r].astype(F32)
            for k in range(n_chan // LANES):
                xt[k, pl.ds(f, n_col, stride=SLOTS), :] = moved[:, k * LANES:(k + 1) * LANES]
        values = jnp.concatenate([xt[k] for k in range(n_chan // LANES)], axis=1)
        hidden[r] = values.astype(BF16)
        for h in range(2):
            part = values[:, h * half:(h + 1) * half]
            ex[0, h, r + 1] = part.astype(BF16)
            cols[0, h, 0, r] = part[0:SLOTS].astype(BF16)
            cols[0, h, 1, r] = part[main - SLOTS:main].astype(BF16)
        for c in range(n_col):
            zt[c * SLOTS:c * SLOTS + n_frame, 0:z_ref.shape[3]] = z_ref[r, c].astype(F32)
        latent = zt[...]
        zx[r + 1] = latent.astype(BF16)
        zcols[0, r] = latent[0:SLOTS].astype(BF16)
        zcols[1, r] = latent[main - SLOTS:main].astype(BF16)
        return carry[0] + tile_sums(values), carry[1] + tile_sums(values * values)

    start_sums = lax.fori_loop(0, n_row, load_row, no_sums(n_chan))

    pl.semaphore_wait(barrier, n_dev - 1)
    z_copies = halo_copies(zx, zcolx, zcols, zsend, zrecv)
    stats_send(0, 0, sum(group_row(h, start_sums[0][:, h * half:(h + 1) * half], start_sums[1][:, h * half:(h + 1) * half]) for h in range(2)))
    for copy in block_halo(0, 0):
        copy.start()
    for copy in z_copies:
        copy.start()
    for copy in block_halo(0, 1):
        copy.start()
    for copy in z_copies:
        copy.wait()

    @pl.loop(0, n_row + 2)
    def _(r):
        zext[r] = jnp.concatenate([zcolx[0, r].astype(F32), zx[r].astype(F32), zcolx[1, r].astype(F32)], axis=0).astype(BF16)

    row_of = lax.broadcasted_iota(jnp.int32, (wide, half), 0)
    slot_of = lax.broadcasted_iota(jnp.int32, (n_col + 2, SLOTS, half), 1)
    first_valid = jnp.where(sw == 0, SLOTS, 0)
    last_valid = jnp.where(sw == n_sw - 1, wide - SLOTS, wide)

    def inside(r):
        beyond = ((r == 0) & (sh == 0)) | ((r == n_row + 1) & (sh == n_sh - 1))
        end = jnp.where(beyond, 0, last_valid)
        return (row_of >= first_valid) & (row_of < end)

    def wide_row(par, h, r):
        return jnp.concatenate([colx[par, h, 0, r].astype(F32), ex[par, h, r].astype(F32), colx[par, h, 1, r].astype(F32)], axis=0)

    frame_of = lax.broadcasted_iota(jnp.int32, (n_col, SLOTS, half), 1).reshape(main, half)

    def activate(i, par, h):
        if h == 0:
            row = 0
            stats_wait(par, 0)
        else:
            row = jnp.minimum(i, 1)

            @pl.when(i > 0)
            def _():
                stats_wait(par, 1)

        total = stat_all[par, row, 0]
        for d in range(1, n_dev):
            total = total + stat_all[par, row, d]
        total = total / count
        group_var = jnp.maximum(pltpu.roll(total, LANES // 2, 1) - total * total, 0.0)
        parts = contract_lanes(limbs(jnp.concatenate([total, lax.rsqrt(group_var + GN_EPSILON)], axis=0)), group[h, 0:half])
        chan_both = parts[0:2] + parts[2:4] + parts[4:6]
        mean = chan_both[0:1]
        scale = chan_both[1:2] * vector(gain_ref, i, h)
        shift = vector(shift_ref, i, h)
        for copy in block_halo(par, h):
            copy.wait()

        @pl.loop(0, n_row + 2)
        def _(r):
            normed = (wide_row(par, h, r) - mean) * scale + shift
            mixed = normed * yb[r, :, h * half:(h + 1) * half] + yb[r, :, n_chan + h * half:n_chan + (h + 1) * half]
            act = jnp.where(inside(r), mixed * jax.nn.sigmoid(mixed), 0.0)
            taps = act.reshape(n_col + 2, SLOTS, half)
            for kt in (2, 1, 0):
                for dw in range(3):
                    xk[h, kt, r, :, dw * half:(dw + 1) * half] = taps[dw:dw + n_col].reshape(main, half).astype(BF16)
                if kt > 0:
                    taps = jnp.where(slot_of == 0, taps, pltpu.roll(taps, 1, 1))

    def taps_of(h):
        return jnp.concatenate([xk[h, kt, dh:dh + n_row].reshape(n_row * main, 3 * half) for kt in range(3) for dh in range(3)], axis=1)

    def weights_of(g, chans):
        return jnp.concatenate([wbuf[(g + kt) % RING, tap, chans] for kt in range(3) for tap in range(9)], axis=1)

    def conv_step(i, _):
        par = i % 2
        after = (i + 1) % 2
        g = 6 * i

        wyb[0:zyw_ref.shape[1], 0:n_chan] = zyw_ref[i]
        wyb[0:zyw_ref.shape[1], n_chan:2 * n_chan] = zbw_ref[i]
        maps = jnp.dot(zext[...].reshape((n_row + 2) * wide, LANES), wyb[...], preferred_element_type=F32)
        map_bias = jnp.concatenate([vector(ref, i, h) for ref in (zyb_ref, zbb_ref) for h in range(2)], axis=1)
        yb[...] = (maps + map_bias).reshape(n_row + 2, wide, 2 * n_chan)

        activate(i, par, 0)
        for kt in range(3):
            weight_wait(g + kt)
        acc[...] = contract_lanes(taps_of(0), weights_of(g, slice(None)))

        @pl.when(i < n_conv - 1)
        def _():
            conv_weights(i + 1, 1)

        activate(i, par, 1)
        for kt in range(3):
            weight_wait(g + 3 + kt)

        second = i % 2 == 1

        def out_half(o, _):
            chans = pl.ds(pl.multiple_of(o * half, half), half)
            acc[:, chans] = acc[:, chans] + contract_lanes(taps_of(1), weights_of(g + 3, chans))
            bias = cb_ref[i // 2, pl.ds(i % 2, 1), chans]

            def finish_row(r, carry):
                conv = (acc[pl.ds(pl.multiple_of(r * main, main), main), chans] + bias).astype(BF16).astype(F32)
                old = hidden[r, :, chans].astype(F32)
                value = jnp.where(second, old + conv, conv).astype(BF16).astype(F32)
                value = jnp.where(frame_of < n_frame, value, 0.0)
                hidden[r, :, chans] = jnp.where(second, value, old).astype(BF16)
                ex[after, o, r + 1] = value.astype(BF16)
                cols[after, o, 0, r] = value[0:SLOTS].astype(BF16)
                cols[after, o, 1, r] = value[main - SLOTS:main].astype(BF16)
                return carry[0] + tile_sums(value), carry[1] + tile_sums(value * value)

            sums = lax.fori_loop(0, n_row, finish_row, no_sums(half))
            copies = block_halo(after, o)
            for copy in copies[0:2]:
                copy.start()

            @pl.when(i < n_conv - 1)
            def _():
                stats_send(after, o, group_row(o, *sums))

            for copy in copies[2:]:
                copy.start()
            return 0

        lax.fori_loop(0, 2, out_half, 0)

        @pl.when(i < n_conv - 2)
        def _():
            conv_weights(i + 2, 0)

        @pl.when(i == n_conv - 2)
        def _():
            up_weights()

        return 0

    lax.fori_loop(0, n_conv, conv_step, 0)

    par = n_conv % 2

    def edges(h):
        for copy in block_halo(par, h):
            copy.wait()

        @pl.loop(0, n_row + 2)
        def _(r):
            value = jnp.where(inside(r), wide_row(par, h, r), 0.0).astype(BF16)
            xk[h, 0, r, :, 0:half] = value[0:main]
            xk[h, 1, r, 0:2 * SLOTS, 0:half] = value[main:wide]

    def products(h, dy):
        begin = jnp.minimum(dy, 1)
        rows = pl.ds(begin, n_row + 1)
        lhs = jnp.concatenate([xk[h, 0, rows, :, 0:half], xk[h, 1, rows, 0:2 * SLOTS, 0:half]], axis=1)
        lhs = lhs.reshape((n_row + 1) * wide, half)
        for dx in range(3):
            w = wbuf[(last_group + h) % RING, dy * 3 + dx]
            product = contract_lanes(lhs, w).reshape(n_row + 1, wide, n_chan)
            lanes = slice(dx * n_chan, (dx + 1) * n_chan)
            prod[dy, :, :, lanes] = product if h == 0 else prod[dy, :, :, lanes] + product

    for h in range(2):
        edges(h)
        weight_wait(last_group + h)

        @pl.loop(0, 3)
        def _(dy):
            products(h, dy)

    up_bias = ub_ref[...]

    @pl.loop(0, n_row)
    def _(r):
        for py in range(2):
            def of(dx, lo):
                at = (slice(lo, lo + main), slice(dx * n_chan, (dx + 1) * n_chan))
                return prod[(0, r + py) + at] + prod[(1, r) + at] + prod[(2, r + py) + at]

            middle = of(1, SLOTS) + up_bias
            phases = [of(0, 0) + middle + of(2, SLOTS), of(0, SLOTS) + middle + of(2, 2 * SLOTS)]
            tiles = [phases[px][c * SLOTS:(c + 1) * SLOTS] for c in range(n_col) for px in range(2)]
            y_ref[2 * r + py] = jnp.concatenate(tiles, axis=0).astype(BF16)


def solution(mesh):
    n_sh = mesh.shape["sh"]
    n_sw = mesh.shape["sw"]

    def local_step(features, latent, gn_gain, gn_bias, zy_weight, zy_bias, zb_weight, zb_bias, conv_weight, conv_bias, up_weight, up_bias):
        _, n_chan, n_frame, n_row, n_col = features.shape
        n_latent = latent.shape[1]
        n_conv = gn_gain.shape[0] * gn_gain.shape[1]
        main = n_col * SLOTS
        wide = main + 2 * SLOTS
        n_dev = n_sh * n_sw
        half = n_chan // 2

        small = lambda values: values.reshape(n_conv, n_latent, n_chan)
        taps = jnp.transpose(conv_weight, (0, 1, 4, 5, 6, 2, 3)).reshape(3 * n_conv, 9, n_chan, n_chan)
        up_taps = jnp.transpose(up_weight, (2, 3, 0, 1)).reshape(9, n_chan, n_chan)
        dims = (n_sh, n_sw, n_frame, n_row, n_col, n_chan, n_conv)
        vmem = pl.BlockSpec(memory_space=pltpu.VMEM)
        hbm = pl.BlockSpec(memory_space=pl.ANY)
        dma = pltpu.SemaphoreType.DMA
        rows = n_row + 2
        result = pl.pallas_call(
            functools.partial(block_kernel, dims),
            out_shape=jax.ShapeDtypeStruct((2 * n_row, 2 * main, n_chan), BF16),
            in_specs=[vmem] * 8 + [hbm, vmem, hbm, vmem],
            out_specs=vmem,
            scratch_shapes=[
                pltpu.VMEM((2, 2, rows, main, half), BF16),
                pltpu.VMEM((2, 2, 2, rows, SLOTS, half), BF16),
                pltpu.VMEM((2, 2, 2, n_row, SLOTS, half), BF16),
                pltpu.VMEM((rows, main, LANES), BF16),
                pltpu.VMEM((2, rows, SLOTS, LANES), BF16),
                pltpu.VMEM((2, n_row, SLOTS, LANES), BF16),
                pltpu.VMEM((rows, wide, LANES), BF16),
                pltpu.VMEM((2, 2, n_dev, 1, LANES), F32),
                pltpu.VMEM((2, n_chan, LANES), BF16),
                pltpu.VMEM((LANES, 2 * n_chan), BF16),
                pltpu.VMEM((rows, wide, 2 * n_chan), F32),
                pltpu.VMEM((2, 3, rows, main, 3 * half), BF16),
                pltpu.VMEM((n_row * main, n_chan), F32),
                pltpu.VMEM((n_row, main, n_chan), BF16),
                pltpu.VMEM((RING, 9, n_chan, half), BF16),
                pltpu.VMEM((3, n_row + 1, wide, 3 * n_chan), F32),
                pltpu.VMEM((n_chan // LANES, main, LANES), F32),
                pltpu.VMEM((main, LANES), F32),
                dma((RING,)),
                dma((2, 2, 8)),
                dma((2, 2, 8)),
                dma((8,)),
                dma((8,)),
                dma((2, 2)),
                dma((2, 2)),
            ],
            compiler_params=pltpu.CompilerParams(collective_id=0, has_side_effects=True, vmem_limit_bytes=64 * 1024 * 1024 - 65536 - 4096),
            name="decoder_block",
        )(jnp.transpose(features[0], (1, 2, 3, 0)), jnp.transpose(latent[0], (2, 3, 1, 0)), gn_gain, gn_bias, small(zy_weight), zy_bias,
          small(zb_weight), zb_bias, taps, conv_bias, up_taps, up_bias.reshape(1, n_chan))
        frames = result.reshape(2 * n_row, 2 * n_col, SLOTS, n_chan)[:, :, :n_frame]
        return jnp.transpose(frames, (3, 2, 0, 1))[None]

    data_spec = P("dp", None, None, "sh", "sw")
    return jax.shard_map(local_step, mesh=mesh, in_specs=(data_spec, data_spec) + (P(),) * 10, out_specs=data_spec, check_vma=False)
```

```python
import functools

import jax
import jax.numpy as jnp
from jax import lax
from jax.experimental import pallas as pl
from jax.experimental.pallas import tpu as pltpu
from jax.sharding import PartitionSpec as P

NUM_GROUPS = 32
GN_EPSILON = 1e-6
LANES = 128
SLOTS = 8
RING = 9
MESH = pl.DeviceIdType.MESH
F32 = jnp.float32
BF16 = jnp.bfloat16


def limbs(values):
    high = values.astype(BF16)
    rest = values - high.astype(F32)
    mid = rest.astype(BF16)
    low = (rest - mid.astype(F32)).astype(BF16)
    n = values.shape[0]
    pad = jnp.zeros((16 - 3 * n, values.shape[1]), F32)
    return jnp.concatenate([high.astype(F32), mid.astype(F32), low.astype(F32), pad], axis=0).astype(BF16)


def contract_lanes(a, b):
    return lax.dot_general(a, b, (((1,), (1,)), ((), ())), preferred_element_type=F32)


def block_kernel(dims, x_ref, z_ref, gain_ref, shift_ref, zyw_ref, zyb_ref, zbw_ref, zbb_ref, cw_ref, cb_ref, uw_ref, ub_ref, y_ref,
                 ex, colx, cols, zx, zcolx, zcols, zext, stat_all, group, wyb, yb, xk, acc, hidden, wbuf, prod, xt, zs, zt, ybuf,
                 wsem, hsend, hrecv, zsend, zrecv, ssend, srecv):
    n_sh, n_sw, n_frame, n_row, n_col, n_chan, n_conv = dims
    half = n_chan // 2
    main = n_col * SLOTS
    wide = (n_col + 2) * SLOTS
    n_dev = n_sh * n_sw
    per_group = n_chan // NUM_GROUPS
    count = per_group * n_frame * n_row * n_col * n_dev
    sh = lax.axis_index("sh")
    sw = lax.axis_index("sw")
    me = sw * n_sh + sh
    up, down = (sh + n_sh - 1) % n_sh, (sh + 1) % n_sh
    left, right = (sw + n_sw - 1) % n_sw, (sw + 1) % n_sw

    barrier = pltpu.get_barrier_semaphore()
    hops = lambda a, b: min(a, n_sw - a) + min(b, n_sh - b) / 2
    offsets = sorted(((a, b) for a in range(n_sw) for b in range(n_sh)), key=lambda ab: -hops(*ab))[:-1]
    rows_of, cols_of = [(sh + b) % n_sh for b in range(n_sh)], [(sw + a) % n_sw for a in range(n_sw)]
    peers = [{"sh": rows_of[b], "sw": cols_of[a]} for a, b in offsets]
    for peer in peers:
        pl.semaphore_signal(barrier, inc=1, device_id=peer, device_id_type=MESH)

    last_group = 6 * n_conv

    def conv_weights(i, h):
        for kt in range(3):
            slot = (6 * i + 3 * h + kt) % RING
            pltpu.make_async_copy(cw_ref.at[3 * i + kt, :, :, pl.ds(h * half, half)], wbuf.at[slot], wsem.at[slot]).start()

    def up_weights():
        for h in range(2):
            slot = (last_group + h) % RING
            pltpu.make_async_copy(uw_ref.at[:, :, pl.ds(h * half, half)], wbuf.at[slot], wsem.at[slot]).start()

    def weight_wait(g):
        slot = g % RING
        pltpu.make_async_copy(wbuf.at[slot], wbuf.at[slot], wsem.at[slot]).wait()

    conv_weights(0, 0)
    conv_weights(0, 1)
    conv_weights(1, 0)

    def halo_copies(rows, recv_cols, send_cols, send_sem, recv_sem):
        table = [
            (send_cols.at[0], recv_cols.at[1, pl.ds(1, n_row)], {"sw": left}),
            (send_cols.at[1], recv_cols.at[0, pl.ds(1, n_row)], {"sw": right}),
            (rows.at[1], rows.at[n_row + 1], {"sh": up}),
            (rows.at[n_row], rows.at[0], {"sh": down}),
            (send_cols.at[0, 0], recv_cols.at[1, n_row + 1], {"sh": up, "sw": left}),
            (send_cols.at[1, 0], recv_cols.at[0, n_row + 1], {"sh": up, "sw": right}),
            (send_cols.at[0, n_row - 1], recv_cols.at[1, 0], {"sh": down, "sw": left}),
            (send_cols.at[1, n_row - 1], recv_cols.at[0, 0], {"sh": down, "sw": right}),
        ]
        return [pltpu.make_async_remote_copy(src_ref=src, dst_ref=dst, send_sem=send_sem.at[k], recv_sem=recv_sem.at[k],
                                             device_id=where, device_id_type=MESH) for k, (src, dst, where) in enumerate(table)]

    def block_halo(par, h):
        return halo_copies(ex.at[par, h], colx.at[par, h], cols.at[par, h], hsend.at[par, h], hrecv.at[par, h])

    def group_row(h, first_sum, second_sum):
        both = jnp.concatenate([jnp.sum(first_sum, axis=0, keepdims=True), jnp.sum(second_sum, axis=0, keepdims=True)], axis=1)
        parts = jnp.dot(limbs(both), group[h], preferred_element_type=F32)
        return parts[0:1] + parts[1:2] + parts[2:3]

    def stats_send(par, h, row):
        stat_all[par, h, me] = row
        for peer in peers:
            pltpu.make_async_remote_copy(src_ref=stat_all.at[par, h, me], dst_ref=stat_all.at[par, h, me], send_sem=ssend.at[par, h],
                                         recv_sem=srecv.at[par, h], device_id=peer, device_id_type=MESH).start()

    def stats_wait(par, h):
        several = stat_all.at[par, h, pl.ds(0, n_dev - 1)]
        pltpu.make_async_copy(several, several, srecv.at[par, h]).wait()
        pltpu.make_async_copy(several, several, ssend.at[par, h]).wait()

    def vector(ref, i, h):
        return ref[i // 2, pl.ds(i % 2, 1), h * half:(h + 1) * half]

    chan = lax.broadcasted_iota(jnp.int32, (2 * half, LANES), 0)
    lane = lax.broadcasted_iota(jnp.int32, (2 * half, LANES), 1)
    squares = lane >= LANES // 2
    for h in range(2):
        first = jnp.where(squares, lane - LANES // 2, lane) * per_group - h * half
        held = (first >= 0) & (first < half)
        first = first + jnp.where(squares, half, 0)
        group[h] = jnp.where(held & (chan >= first) & (chan < first + per_group), 1.0, 0.0).astype(BF16)
    wyb[...] = jnp.zeros_like(wyb)
    xt[...] = jnp.zeros_like(xt)
    zs[...] = jnp.zeros_like(zs)
    zt[...] = jnp.zeros_like(zt)

    n_latent = z_ref.shape[2]
    for f in range(n_frame):
        for c in range(n_col):
            k = (f * n_col + c) * n_latent
            zs[k:k + n_latent, 0:n_row] = z_ref[f, c].astype(F32)
    turned = zs[...].T
    for f in range(n_frame):
        for c in range(n_col):
            block, lane_at = divmod((f * n_col + c) * n_latent, LANES)
            moved = turned[0:2 * SLOTS, block * LANES:(block + 1) * LANES]
            if lane_at:
                moved = pltpu.roll(moved, LANES - lane_at, 1)
            zt[pl.ds(c * SLOTS + f, n_row, stride=main), :] = moved[0:n_row]

    def tile_sums(values):
        total = values[0:SLOTS]
        for c in range(1, n_col):
            total = total + values[c * SLOTS:(c + 1) * SLOTS]
        return total

    def no_sums(width):
        return jnp.zeros((SLOTS, width), F32), jnp.zeros((SLOTS, width), F32)

    def load_row(r, carry):
        for f in range(n_frame):
            moved = x_ref[f, r].astype(F32)
            for k in range(n_chan // LANES):
                xt[k, pl.ds(f, n_col, stride=SLOTS), :] = moved[:, k * LANES:(k + 1) * LANES]
        values = jnp.concatenate([xt[k] for k in range(n_chan // LANES)], axis=1)
        hidden[r] = values.astype(BF16)
        for h in range(2):
            part = values[:, h * half:(h + 1) * half]
            ex[0, h, r + 1] = part.astype(BF16)
            cols[0, h, 0, r] = part[0:SLOTS].astype(BF16)
            cols[0, h, 1, r] = part[main - SLOTS:main].astype(BF16)
        latent = zt[pl.ds(pl.multiple_of(r * main, main), main), :]
        zx[r + 1] = latent.astype(BF16)
        zcols[0, r] = latent[0:SLOTS].astype(BF16)
        zcols[1, r] = latent[main - SLOTS:main].astype(BF16)
        return carry[0] + tile_sums(values), carry[1] + tile_sums(values * values)

    start_sums = lax.fori_loop(0, n_row, load_row, no_sums(n_chan))

    pl.semaphore_wait(barrier, n_dev - 1)
    z_copies = halo_copies(zx, zcolx, zcols, zsend, zrecv)
    stats_send(0, 0, sum(group_row(h, start_sums[0][:, h * half:(h + 1) * half], start_sums[1][:, h * half:(h + 1) * half]) for h in range(2)))
    for copy in block_halo(0, 0):
        copy.start()
    for copy in z_copies:
        copy.start()
    for copy in block_halo(0, 1):
        copy.start()
    for copy in z_copies:
        copy.wait()

    @pl.loop(0, n_row + 2)
    def _(r):
        zext[r] = jnp.concatenate([zcolx[0, r].astype(F32), zx[r].astype(F32), zcolx[1, r].astype(F32)], axis=0).astype(BF16)

    row_of = lax.broadcasted_iota(jnp.int32, (wide, half), 0)
    slot_of = lax.broadcasted_iota(jnp.int32, (n_col + 2, SLOTS, half), 1)
    first_valid = jnp.where(sw == 0, SLOTS, 0)
    last_valid = jnp.where(sw == n_sw - 1, wide - SLOTS, wide)

    def inside(r):
        beyond = ((r == 0) & (sh == 0)) | ((r == n_row + 1) & (sh == n_sh - 1))
        end = jnp.where(beyond, 0, last_valid)
        return (row_of >= first_valid) & (row_of < end)

    def wide_row(par, h, r):
        return jnp.concatenate([colx[par, h, 0, r].astype(F32), ex[par, h, r].astype(F32), colx[par, h, 1, r].astype(F32)], axis=0)

    frame_of = lax.broadcasted_iota(jnp.int32, (n_col, SLOTS, half), 1).reshape(main, half)

    def activate(i, par, h):
        if h == 0:
            row = 0
            stats_wait(par, 0)
        else:
            row = jnp.minimum(i, 1)

            @pl.when(i > 0)
            def _():
                stats_wait(par, 1)

        total = stat_all[par, row, 0]
        for d in range(1, n_dev):
            total = total + stat_all[par, row, d]
        total = total / count
        group_var = jnp.maximum(pltpu.roll(total, LANES // 2, 1) - total * total, 0.0)
        parts = contract_lanes(limbs(jnp.concatenate([total, lax.rsqrt(group_var + GN_EPSILON)], axis=0)), group[h, 0:half])
        chan_both = parts[0:2] + parts[2:4] + parts[4:6]
        mean = chan_both[0:1]
        scale = chan_both[1:2] * vector(gain_ref, i, h)
        shift = vector(shift_ref, i, h)
        for copy in block_halo(par, h):
            copy.wait()

        @pl.loop(0, n_row + 2)
        def _(r):
            normed = (wide_row(par, h, r) - mean) * scale + shift
            mixed = normed * yb[r, :, h * half:(h + 1) * half] + yb[r, :, n_chan + h * half:n_chan + (h + 1) * half]
            act = jnp.where(inside(r), mixed * jax.nn.sigmoid(mixed), 0.0)
            taps = act.reshape(n_col + 2, SLOTS, half)
            for kt in (2, 1, 0):
                for dw in range(3):
                    xk[h, kt, r, :, dw * half:(dw + 1) * half] = taps[dw:dw + n_col].reshape(main, half).astype(BF16)
                if kt > 0:
                    taps = jnp.where(slot_of == 0, taps, pltpu.roll(taps, 1, 1))

    def taps_of(h):
        return jnp.concatenate([xk[h, kt, dh:dh + n_row].reshape(n_row * main, 3 * half) for kt in range(3) for dh in range(3)], axis=1)

    def weights_of(g, chans):
        return jnp.concatenate([wbuf[(g + kt) % RING, tap, chans] for kt in range(3) for tap in range(9)], axis=1)

    def conv_step(i, _):
        par = i % 2
        after = (i + 1) % 2
        g = 6 * i

        wyb[0:n_latent, 0:n_chan] = zyw_ref[i]
        wyb[0:n_latent, n_chan:2 * n_chan] = zbw_ref[i]
        maps = jnp.dot(zext[...].reshape((n_row + 2) * wide, LANES), wyb[...], preferred_element_type=F32)
        map_bias = jnp.concatenate([vector(ref, i, h) for ref in (zyb_ref, zbb_ref) for h in range(2)], axis=1)
        yb[...] = (maps + map_bias).reshape(n_row + 2, wide, 2 * n_chan)

        activate(i, par, 0)
        for kt in range(3):
            weight_wait(g + kt)
        acc[...] = contract_lanes(taps_of(0), weights_of(g, slice(None)))

        @pl.when(i < n_conv - 1)
        def _():
            conv_weights(i + 1, 1)

        activate(i, par, 1)
        for kt in range(3):
            weight_wait(g + 3 + kt)

        second = i % 2 == 1

        def out_half(o, _):
            chans = pl.ds(pl.multiple_of(o * half, half), half)
            acc[:, chans] = acc[:, chans] + contract_lanes(taps_of(1), weights_of(g + 3, chans))
            bias = cb_ref[i // 2, pl.ds(i % 2, 1), chans]

            def finish_row(r, carry):
                conv = (acc[pl.ds(pl.multiple_of(r * main, main), main), chans] + bias).astype(BF16).astype(F32)
                old = hidden[r, :, chans].astype(F32)
                value = jnp.where(second, old + conv, conv).astype(BF16).astype(F32)
                value = jnp.where(frame_of < n_frame, value, 0.0)
                hidden[r, :, chans] = jnp.where(second, value, old).astype(BF16)
                ex[after, o, r + 1] = value.astype(BF16)
                cols[after, o, 0, r] = value[0:SLOTS].astype(BF16)
                cols[after, o, 1, r] = value[main - SLOTS:main].astype(BF16)
                return carry[0] + tile_sums(value), carry[1] + tile_sums(value * value)

            sums = lax.fori_loop(0, n_row, finish_row, no_sums(half))
            copies = block_halo(after, o)
            for copy in copies[0:2]:
                copy.start()

            @pl.when(i < n_conv - 1)
            def _():
                stats_send(after, o, group_row(o, *sums))

            for copy in copies[2:]:
                copy.start()
            return 0

        lax.fori_loop(0, 2, out_half, 0)

        @pl.when(i < n_conv - 2)
        def _():
            conv_weights(i + 2, 0)

        @pl.when(i == n_conv - 2)
        def _():
            up_weights()

        return 0

    lax.fori_loop(0, n_conv, conv_step, 0)

    par = n_conv % 2

    def edges(h):
        for copy in block_halo(par, h):
            copy.wait()

        @pl.loop(0, n_row + 2)
        def _(r):
            value = jnp.where(inside(r), wide_row(par, h, r), 0.0).astype(BF16)
            xk[h, 0, r, :, 0:half] = value[0:main]
            xk[h, 1, r, 0:2 * SLOTS, 0:half] = value[main:wide]

    def products(h, dy):
        begin = jnp.minimum(dy, 1)
        rows = pl.ds(begin, n_row + 1)
        lhs = jnp.concatenate([xk[h, 0, rows, :, 0:half], xk[h, 1, rows, 0:2 * SLOTS, 0:half]], axis=1)
        lhs = lhs.reshape((n_row + 1) * wide, half)
        for dx in range(3):
            w = wbuf[(last_group + h) % RING, dy * 3 + dx]
            product = contract_lanes(lhs, w).reshape(n_row + 1, wide, n_chan)
            lanes = slice(dx * n_chan, (dx + 1) * n_chan)
            prod[dy, :, :, lanes] = product if h == 0 else prod[dy, :, :, lanes] + product

    for h in range(2):
        edges(h)
        weight_wait(last_group + h)

        @pl.loop(0, 3)
        def _(dy):
            products(h, dy)

    up_bias = ub_ref[...]

    @pl.loop(0, n_row)
    def _(r):
        for py in range(2):
            def of(dx, lo):
                at = (slice(lo, lo + main), slice(dx * n_chan, (dx + 1) * n_chan))
                return prod[(0, r + py) + at] + prod[(1, r) + at] + prod[(2, r + py) + at]

            middle = of(1, SLOTS) + up_bias
            phases = [of(0, 0) + middle + of(2, SLOTS), of(0, SLOTS) + middle + of(2, 2 * SLOTS)]
            for c in range(n_col):
                for px in range(2):
                    tile = phases[px][c * SLOTS:(c + 1) * SLOTS]
                    for k in range(n_chan // LANES):
                        rows = pl.ds((2 * c + px) * SLOTS * 2 * n_row + 2 * r + py, SLOTS, stride=2 * n_row)
                        ybuf[k, rows, :] = tile[:, k * LANES:(k + 1) * LANES]

    @pl.loop(0, 2 * n_col)
    def _(c):
        for f in range(n_frame):
            rows = pl.ds(pl.multiple_of((c * SLOTS + f) * 2 * n_row, SLOTS), 2 * n_row)
            y_ref[f, c] = jnp.concatenate([ybuf[k, rows, :] for k in range(n_chan // LANES)], axis=1).astype(BF16)


def solution(mesh):
    n_sh = mesh.shape["sh"]
    n_sw = mesh.shape["sw"]

    def local_step(features, latent, gn_gain, gn_bias, zy_weight, zy_bias, zb_weight, zb_bias, conv_weight, conv_bias, up_weight, up_bias):
        _, n_chan, n_frame, n_row, n_col = features.shape
        n_latent = latent.shape[1]
        n_conv = gn_gain.shape[0] * gn_gain.shape[1]
        main = n_col * SLOTS
        wide = main + 2 * SLOTS
        n_dev = n_sh * n_sw
        half = n_chan // 2

        small = lambda values: values.reshape(n_conv, n_latent, n_chan)
        taps = jnp.transpose(conv_weight, (0, 1, 4, 5, 6, 2, 3)).reshape(3 * n_conv, 9, n_chan, n_chan)
        up_taps = jnp.transpose(up_weight, (2, 3, 0, 1)).reshape(9, n_chan, n_chan)
        dims = (n_sh, n_sw, n_frame, n_row, n_col, n_chan, n_conv)
        vmem = pl.BlockSpec(memory_space=pltpu.VMEM)
        hbm = pl.BlockSpec(memory_space=pl.ANY)
        dma = pltpu.SemaphoreType.DMA
        rows = n_row + 2
        result = pl.pallas_call(
            functools.partial(block_kernel, dims),
            out_shape=jax.ShapeDtypeStruct((n_frame, 2 * n_col, 2 * n_row, n_chan), BF16),
            in_specs=[vmem] * 8 + [hbm, vmem, hbm, vmem],
            out_specs=vmem,
            scratch_shapes=[
                pltpu.VMEM((2, 2, rows, main, half), BF16),
                pltpu.VMEM((2, 2, 2, rows, SLOTS, half), BF16),
                pltpu.VMEM((2, 2, 2, n_row, SLOTS, half), BF16),
                pltpu.VMEM((rows, main, LANES), BF16),
                pltpu.VMEM((2, rows, SLOTS, LANES), BF16),
                pltpu.VMEM((2, n_row, SLOTS, LANES), BF16),
                pltpu.VMEM((rows, wide, LANES), BF16),
                pltpu.VMEM((2, 2, n_dev, 1, LANES), F32),
                pltpu.VMEM((2, n_chan, LANES), BF16),
                pltpu.VMEM((LANES, 2 * n_chan), BF16),
                pltpu.VMEM((rows, wide, 2 * n_chan), F32),
                pltpu.VMEM((2, 3, rows, main, 3 * half), BF16),
                pltpu.VMEM((n_row * main, n_chan), F32),
                pltpu.VMEM((n_row, main, n_chan), BF16),
                pltpu.VMEM((RING, 9, n_chan, half), BF16),
                pltpu.VMEM((3, n_row + 1, wide, 3 * n_chan), F32),
                pltpu.VMEM((n_chan // LANES, main, LANES), F32),
                pltpu.VMEM((pl.cdiv(n_frame * n_col * n_latent, LANES) * LANES, LANES), F32),
                pltpu.VMEM((n_row * main, LANES), F32),
                pltpu.VMEM((n_chan // LANES, 2 * n_col * SLOTS * 2 * n_row, LANES), F32),
                dma((RING,)),
                dma((2, 2, 8)),
                dma((2, 2, 8)),
                dma((8,)),
                dma((8,)),
                dma((2, 2)),
                dma((2, 2)),
            ],
            compiler_params=pltpu.CompilerParams(collective_id=0, has_side_effects=True, vmem_limit_bytes=64 * 1024 * 1024 - 65536 - 4096),
            name="decoder_block",
        )(jnp.transpose(features[0], (1, 2, 3, 0)), jnp.transpose(latent[0], (1, 3, 0, 2)), gn_gain, gn_bias, small(zy_weight), zy_bias,
          small(zb_weight), zb_bias, taps, conv_bias, up_taps, up_bias.reshape(1, n_chan))
        return jnp.transpose(result, (3, 0, 2, 1))[None]

    data_spec = P("dp", None, None, "sh", "sw")
    return jax.shard_map(local_step, mesh=mesh, in_specs=(data_spec, data_spec) + (P(),) * 10, out_specs=data_spec, check_vma=False)
```

```python
import functools

import jax
import jax.numpy as jnp
from jax import lax
from jax.experimental import pallas as pl
from jax.experimental.pallas import tpu as pltpu
from jax.sharding import PartitionSpec as P

NUM_GROUPS = 32
GN_EPSILON = 1e-6
LANES = 128
SLOTS = 8
RING = 9
MESH = pl.DeviceIdType.MESH
F32 = jnp.float32
BF16 = jnp.bfloat16


def limbs(values):
    high = values.astype(BF16)
    rest = values - high.astype(F32)
    mid = rest.astype(BF16)
    low = (rest - mid.astype(F32)).astype(BF16)
    n = values.shape[0]
    pad = jnp.zeros((16 - 3 * n, values.shape[1]), F32)
    return jnp.concatenate([high.astype(F32), mid.astype(F32), low.astype(F32), pad], axis=0).astype(BF16)


def contract_lanes(a, b):
    return lax.dot_general(a, b, (((1,), (1,)), ((), ())), preferred_element_type=F32)


def block_kernel(dims, x_ref, z_ref, gain_ref, shift_ref, zyw_ref, zyb_ref, zbw_ref, zbb_ref, cw_ref, cb_ref, uw_ref, ub_ref, y_ref,
                 ex, colx, cols, zx, zcolx, zcols, zext, stat_all, group, wyb, yb, xk, acc, hidden, wbuf, prod, xt, zs, zt, ybuf,
                 wsem, hsend, hrecv, zsend, zrecv, ssend, srecv):
    n_sh, n_sw, n_frame, n_row, n_col, n_chan, n_conv = dims
    half = n_chan // 2
    main = n_col * SLOTS
    wide = (n_col + 2) * SLOTS
    n_dev = n_sh * n_sw
    per_group = n_chan // NUM_GROUPS
    count = per_group * n_frame * n_row * n_col * n_dev
    sh = lax.axis_index("sh")
    sw = lax.axis_index("sw")
    me = sw * n_sh + sh
    up, down = (sh + n_sh - 1) % n_sh, (sh + 1) % n_sh
    left, right = (sw + n_sw - 1) % n_sw, (sw + 1) % n_sw

    barrier = pltpu.get_barrier_semaphore()
    hops = lambda a, b: min(a, n_sw - a) + min(b, n_sh - b) / 2
    offsets = sorted(((a, b) for a in range(n_sw) for b in range(n_sh)), key=lambda ab: -hops(*ab))[:-1]
    rows_of, cols_of = [(sh + b) % n_sh for b in range(n_sh)], [(sw + a) % n_sw for a in range(n_sw)]
    peers = [{"sh": rows_of[b], "sw": cols_of[a]} for a, b in offsets]
    for peer in peers:
        pl.semaphore_signal(barrier, inc=1, device_id=peer, device_id_type=MESH)

    last_group = 6 * n_conv

    def conv_weights(i, h):
        for kt in range(3):
            slot = (6 * i + 3 * h + kt) % RING
            pltpu.make_async_copy(cw_ref.at[3 * i + kt, :, :, pl.ds(h * half, half)], wbuf.at[slot], wsem.at[slot]).start()

    def up_weights():
        for h in range(2):
            slot = (last_group + h) % RING
            pltpu.make_async_copy(uw_ref.at[:, :, pl.ds(h * half, half)], wbuf.at[slot], wsem.at[slot]).start()

    def weight_wait(g):
        slot = g % RING
        pltpu.make_async_copy(wbuf.at[slot], wbuf.at[slot], wsem.at[slot]).wait()

    conv_weights(0, 0)
    conv_weights(0, 1)
    conv_weights(1, 0)

    def halo_copies(rows, recv_cols, send_cols, send_sem, recv_sem):
        table = [
            (send_cols.at[0], recv_cols.at[1, pl.ds(1, n_row)], {"sw": left}),
            (send_cols.at[1], recv_cols.at[0, pl.ds(1, n_row)], {"sw": right}),
            (rows.at[1], rows.at[n_row + 1], {"sh": up}),
            (rows.at[n_row], rows.at[0], {"sh": down}),
            (send_cols.at[0, 0], recv_cols.at[1, n_row + 1], {"sh": up, "sw": left}),
            (send_cols.at[1, 0], recv_cols.at[0, n_row + 1], {"sh": up, "sw": right}),
            (send_cols.at[0, n_row - 1], recv_cols.at[1, 0], {"sh": down, "sw": left}),
            (send_cols.at[1, n_row - 1], recv_cols.at[0, 0], {"sh": down, "sw": right}),
        ]
        return [pltpu.make_async_remote_copy(src_ref=src, dst_ref=dst, send_sem=send_sem.at[k], recv_sem=recv_sem.at[k],
                                             device_id=where, device_id_type=MESH) for k, (src, dst, where) in enumerate(table)]

    def block_halo(par, h):
        return halo_copies(ex.at[par, h], colx.at[par, h], cols.at[par, h], hsend.at[par, h], hrecv.at[par, h])

    def group_row(h, first_sum, second_sum):
        both = jnp.concatenate([jnp.sum(first_sum, axis=0, keepdims=True), jnp.sum(second_sum, axis=0, keepdims=True)], axis=1)
        parts = jnp.dot(limbs(both), group[h], preferred_element_type=F32)
        return parts[0:1] + parts[1:2] + parts[2:3]

    def stats_send(par, h, row):
        stat_all[par, h, me] = row
        for peer in peers:
            pltpu.make_async_remote_copy(src_ref=stat_all.at[par, h, me], dst_ref=stat_all.at[par, h, me], send_sem=ssend.at[par, h],
                                         recv_sem=srecv.at[par, h], device_id=peer, device_id_type=MESH).start()

    def stats_wait(par, h):
        several = stat_all.at[par, h, pl.ds(0, n_dev - 1)]
        pltpu.make_async_copy(several, several, srecv.at[par, h]).wait()
        pltpu.make_async_copy(several, several, ssend.at[par, h]).wait()

    def vector(ref, i, h):
        return ref[i // 2, pl.ds(i % 2, 1), h * half:(h + 1) * half]

    chan = lax.broadcasted_iota(jnp.int32, (2 * half, LANES), 0)
    lane = lax.broadcasted_iota(jnp.int32, (2 * half, LANES), 1)
    squares = lane >= LANES // 2
    for h in range(2):
        first = jnp.where(squares, lane - LANES // 2, lane) * per_group - h * half
        held = (first >= 0) & (first < half)
        first = first + jnp.where(squares, half, 0)
        group[h] = jnp.where(held & (chan >= first) & (chan < first + per_group), 1.0, 0.0).astype(BF16)
    wyb[...] = jnp.zeros_like(wyb)
    xt[...] = jnp.zeros_like(xt)
    zs[...] = jnp.zeros_like(zs)
    zt[...] = jnp.zeros_like(zt)

    n_latent = z_ref.shape[2]
    for f in range(n_frame):
        for c in range(n_col):
            k = (f * n_col + c) * n_latent
            zs[k:k + n_latent, 0:n_row] = z_ref[f, c].astype(F32)
    turned = zs[...].T
    for f in range(n_frame):
        for c in range(n_col):
            block, lane_at = divmod((f * n_col + c) * n_latent, LANES)
            moved = turned[0:2 * SLOTS, block * LANES:(block + 1) * LANES]
            if lane_at:
                moved = pltpu.roll(moved, LANES - lane_at, 1)
            zt[pl.ds(c * SLOTS + f, n_row, stride=main), :] = moved[0:n_row]

    def tile_sums(values):
        total = values[0:SLOTS]
        for c in range(1, n_col):
            total = total + values[c * SLOTS:(c + 1) * SLOTS]
        return total

    def no_sums(width):
        return jnp.zeros((SLOTS, width), F32), jnp.zeros((SLOTS, width), F32)

    def load_row(r, carry):
        for f in range(n_frame):
            moved = x_ref[f, r].astype(F32)
            for k in range(n_chan // LANES):
                xt[k, pl.ds(f, n_col, stride=SLOTS), :] = moved[:, k * LANES:(k + 1) * LANES]
        values = jnp.concatenate([xt[k] for k in range(n_chan // LANES)], axis=1)
        hidden[r] = values.astype(BF16)
        for h in range(2):
            part = values[:, h * half:(h + 1) * half]
            ex[0, h, r + 1] = part.astype(BF16)
            cols[0, h, 0, r] = part[0:SLOTS].astype(BF16)
            cols[0, h, 1, r] = part[main - SLOTS:main].astype(BF16)
        latent = zt[pl.ds(pl.multiple_of(r * main, main), main), :]
        zx[r + 1] = latent.astype(BF16)
        zcols[0, r] = latent[0:SLOTS].astype(BF16)
        zcols[1, r] = latent[main - SLOTS:main].astype(BF16)
        return carry[0] + tile_sums(values), carry[1] + tile_sums(values * values)

    start_sums = lax.fori_loop(0, n_row, load_row, no_sums(n_chan))

    pl.semaphore_wait(barrier, n_dev - 1)
    z_copies = halo_copies(zx, zcolx, zcols, zsend, zrecv)
    stats_send(0, 0, sum(group_row(h, start_sums[0][:, h * half:(h + 1) * half], start_sums[1][:, h * half:(h + 1) * half]) for h in range(2)))
    for copy in block_halo(0, 0):
        copy.start()
    for copy in z_copies:
        copy.start()
    for copy in block_halo(0, 1):
        copy.start()
    for copy in z_copies:
        copy.wait()

    @pl.loop(0, n_row + 2)
    def _(r):
        zext[r] = jnp.concatenate([zcolx[0, r].astype(F32), zx[r].astype(F32), zcolx[1, r].astype(F32)], axis=0).astype(BF16)

    row_of = lax.broadcasted_iota(jnp.int32, (wide, half), 0)
    slot_of = lax.broadcasted_iota(jnp.int32, (n_col + 2, SLOTS, half), 1)
    first_valid = jnp.where(sw == 0, SLOTS, 0)
    last_valid = jnp.where(sw == n_sw - 1, wide - SLOTS, wide)

    def inside(r):
        beyond = ((r == 0) & (sh == 0)) | ((r == n_row + 1) & (sh == n_sh - 1))
        end = jnp.where(beyond, 0, last_valid)
        return (row_of >= first_valid) & (row_of < end)

    def wide_row(par, h, r):
        return jnp.concatenate([colx[par, h, 0, r].astype(F32), ex[par, h, r].astype(F32), colx[par, h, 1, r].astype(F32)], axis=0)

    frame_of = lax.broadcasted_iota(jnp.int32, (n_col, SLOTS, half), 1).reshape(main, half)

    def activate(i, par, h):
        if h == 0:
            row = 0
            stats_wait(par, 0)
        else:
            row = jnp.minimum(i, 1)

            @pl.when(i > 0)
            def _():
                stats_wait(par, 1)

        total = stat_all[par, row, 0]
        for d in range(1, n_dev):
            total = total + stat_all[par, row, d]
        total = total / count
        group_var = jnp.maximum(pltpu.roll(total, LANES // 2, 1) - total * total, 0.0)
        parts = contract_lanes(limbs(jnp.concatenate([total, lax.rsqrt(group_var + GN_EPSILON)], axis=0)), group[h, 0:half])
        chan_both = parts[0:2] + parts[2:4] + parts[4:6]
        mean = chan_both[0:1]
        scale = chan_both[1:2] * vector(gain_ref, i, h)
        shift = vector(shift_ref, i, h)
        for copy in block_halo(par, h):
            copy.wait()

        @pl.loop(0, n_row + 2)
        def _(r):
            normed = (wide_row(par, h, r) - mean) * scale + shift
            mixed = normed * yb[r, :, h * half:(h + 1) * half] + yb[r, :, n_chan + h * half:n_chan + (h + 1) * half]
            act = jnp.where(inside(r), mixed * jax.nn.sigmoid(mixed), 0.0)
            taps = act.reshape(n_col + 2, SLOTS, half)
            for kt in (2, 1, 0):
                for dw in range(3):
                    xk[h, kt, r, :, dw * half:(dw + 1) * half] = taps[dw:dw + n_col].reshape(main, half).astype(BF16)
                if kt > 0:
                    taps = jnp.where(slot_of == 0, taps, pltpu.roll(taps, 1, 1))

    def taps_of(h):
        return jnp.concatenate([xk[h, kt, dh:dh + n_row].reshape(n_row * main, 3 * half) for kt in range(3) for dh in range(3)], axis=1)

    def weights_of(g, chans):
        return jnp.concatenate([wbuf[(g + kt) % RING, tap, chans] for kt in range(3) for tap in range(9)], axis=1)

    def conv_step(i, _):
        par = i % 2
        after = (i + 1) % 2
        g = 6 * i

        wyb[0:n_latent, 0:n_chan] = zyw_ref[i]
        wyb[0:n_latent, n_chan:2 * n_chan] = zbw_ref[i]
        maps = jnp.dot(zext[...].reshape((n_row + 2) * wide, LANES), wyb[...], preferred_element_type=F32)
        map_bias = jnp.concatenate([vector(ref, i, h) for ref in (zyb_ref, zbb_ref) for h in range(2)], axis=1)
        yb[...] = (maps + map_bias).reshape(n_row + 2, wide, 2 * n_chan)

        activate(i, par, 0)
        for kt in range(3):
            weight_wait(g + kt)
        acc[...] = contract_lanes(taps_of(0), weights_of(g, slice(None)))

        @pl.when(i < n_conv - 1)
        def _():
            conv_weights(i + 1, 1)

        activate(i, par, 1)
        for kt in range(3):
            weight_wait(g + 3 + kt)

        second = i % 2 == 1

        def out_half(o, _):
            chans = pl.ds(pl.multiple_of(o * half, half), half)
            part = contract_lanes(taps_of(1), weights_of(g + 3, chans))
            bias = cb_ref[i // 2, pl.ds(i % 2, 1), chans]

            def finish_row(r, carry):
                at = slice(r * main, (r + 1) * main)
                conv = (acc[at, chans] + part[at] + bias).astype(BF16).astype(F32)
                old = hidden[r, :, chans].astype(F32)
                value = jnp.where(second, old + conv, conv).astype(BF16).astype(F32)
                value = jnp.where(frame_of < n_frame, value, 0.0)
                hidden[r, :, chans] = jnp.where(second, value, old).astype(BF16)
                ex[after, o, r + 1] = value.astype(BF16)
                cols[after, o, 0, r] = value[0:SLOTS].astype(BF16)
                cols[after, o, 1, r] = value[main - SLOTS:main].astype(BF16)
                return carry[0] + tile_sums(value), carry[1] + tile_sums(value * value)

            sums = no_sums(half)
            for r in range(n_row):
                sums = finish_row(r, sums)
            copies = block_halo(after, o)
            for copy in copies[0:2]:
                copy.start()

            @pl.when(i < n_conv - 1)
            def _():
                stats_send(after, o, group_row(o, *sums))

            for copy in copies[2:]:
                copy.start()
            return 0

        lax.fori_loop(0, 2, out_half, 0)

        @pl.when(i < n_conv - 2)
        def _():
            conv_weights(i + 2, 0)

        @pl.when(i == n_conv - 2)
        def _():
            up_weights()

        return 0

    lax.fori_loop(0, n_conv, conv_step, 0)

    par = n_conv % 2

    def edges(h):
        for copy in block_halo(par, h):
            copy.wait()

        @pl.loop(0, n_row + 2)
        def _(r):
            value = jnp.where(inside(r), wide_row(par, h, r), 0.0).astype(BF16)
            xk[h, 0, r, :, 0:half] = value[0:main]
            xk[h, 1, r, 0:2 * SLOTS, 0:half] = value[main:wide]

    def products(h, dy):
        begin = jnp.minimum(dy, 1)
        rows = pl.ds(begin, n_row + 1)
        lhs = jnp.concatenate([xk[h, 0, rows, :, 0:half], xk[h, 1, rows, 0:2 * SLOTS, 0:half]], axis=1)
        lhs = lhs.reshape((n_row + 1) * wide, half)
        for dx in range(3):
            w = wbuf[(last_group + h) % RING, dy * 3 + dx]
            product = contract_lanes(lhs, w).reshape(n_row + 1, wide, n_chan)
            lanes = slice(dx * n_chan, (dx + 1) * n_chan)
            prod[dy, :, :, lanes] = product if h == 0 else prod[dy, :, :, lanes] + product

    for h in range(2):
        edges(h)
        weight_wait(last_group + h)

        @pl.loop(0, 3)
        def _(dy):
            products(h, dy)

    up_bias = ub_ref[...]

    @pl.loop(0, n_row)
    def _(r):
        for py in range(2):
            def of(dx, lo):
                at = (slice(lo, lo + main), slice(dx * n_chan, (dx + 1) * n_chan))
                return prod[(0, r + py) + at] + prod[(1, r) + at] + prod[(2, r + py) + at]

            middle = of(1, SLOTS) + up_bias
            phases = [of(0, 0) + middle + of(2, SLOTS), of(0, SLOTS) + middle + of(2, 2 * SLOTS)]
            for c in range(n_col):
                for px in range(2):
                    tile = phases[px][c * SLOTS:(c + 1) * SLOTS]
                    for k in range(n_chan // LANES):
                        rows = pl.ds((2 * c + px) * SLOTS * 2 * n_row + 2 * r + py, SLOTS, stride=2 * n_row)
                        ybuf[k, rows, :] = tile[:, k * LANES:(k + 1) * LANES]

    @pl.loop(0, 2 * n_col)
    def _(c):
        for f in range(n_frame):
            rows = pl.ds(pl.multiple_of((c * SLOTS + f) * 2 * n_row, SLOTS), 2 * n_row)
            y_ref[f, c] = jnp.concatenate([ybuf[k, rows, :] for k in range(n_chan // LANES)], axis=1).astype(BF16)


def solution(mesh):
    n_sh = mesh.shape["sh"]
    n_sw = mesh.shape["sw"]

    def local_step(features, latent, gn_gain, gn_bias, zy_weight, zy_bias, zb_weight, zb_bias, conv_weight, conv_bias, up_weight, up_bias):
        _, n_chan, n_frame, n_row, n_col = features.shape
        n_latent = latent.shape[1]
        n_conv = gn_gain.shape[0] * gn_gain.shape[1]
        main = n_col * SLOTS
        wide = main + 2 * SLOTS
        n_dev = n_sh * n_sw
        half = n_chan // 2

        small = lambda values: values.reshape(n_conv, n_latent, n_chan)
        taps = jnp.transpose(conv_weight, (0, 1, 4, 5, 6, 2, 3)).reshape(3 * n_conv, 9, n_chan, n_chan)
        up_taps = jnp.transpose(up_weight, (2, 3, 0, 1)).reshape(9, n_chan, n_chan)
        dims = (n_sh, n_sw, n_frame, n_row, n_col, n_chan, n_conv)
        vmem = pl.BlockSpec(memory_space=pltpu.VMEM)
        hbm = pl.BlockSpec(memory_space=pl.ANY)
        dma = pltpu.SemaphoreType.DMA
        rows = n_row + 2
        result = pl.pallas_call(
            functools.partial(block_kernel, dims),
            out_shape=jax.ShapeDtypeStruct((n_frame, 2 * n_col, 2 * n_row, n_chan), BF16),
            in_specs=[vmem] * 8 + [hbm, vmem, hbm, vmem],
            out_specs=vmem,
            scratch_shapes=[
                pltpu.VMEM((2, 2, rows, main, half), BF16),
                pltpu.VMEM((2, 2, 2, rows, SLOTS, half), BF16),
                pltpu.VMEM((2, 2, 2, n_row, SLOTS, half), BF16),
                pltpu.VMEM((rows, main, LANES), BF16),
                pltpu.VMEM((2, rows, SLOTS, LANES), BF16),
                pltpu.VMEM((2, n_row, SLOTS, LANES), BF16),
                pltpu.VMEM((rows, wide, LANES), BF16),
                pltpu.VMEM((2, 2, n_dev, 1, LANES), F32),
                pltpu.VMEM((2, n_chan, LANES), BF16),
                pltpu.VMEM((LANES, 2 * n_chan), BF16),
                pltpu.VMEM((rows, wide, 2 * n_chan), F32),
                pltpu.VMEM((2, 3, rows, main, 3 * half), BF16),
                pltpu.VMEM((n_row * main, n_chan), F32),
                pltpu.VMEM((n_row, main, n_chan), BF16),
                pltpu.VMEM((RING, 9, n_chan, half), BF16),
                pltpu.VMEM((3, n_row + 1, wide, 3 * n_chan), F32),
                pltpu.VMEM((n_chan // LANES, main, LANES), F32),
                pltpu.VMEM((pl.cdiv(n_frame * n_col * n_latent, LANES) * LANES, LANES), F32),
                pltpu.VMEM((n_row * main, LANES), F32),
                pltpu.VMEM((n_chan // LANES, 2 * n_col * SLOTS * 2 * n_row, LANES), F32),
                dma((RING,)),
                dma((2, 2, 8)),
                dma((2, 2, 8)),
                dma((8,)),
                dma((8,)),
                dma((2, 2)),
                dma((2, 2)),
            ],
            compiler_params=pltpu.CompilerParams(collective_id=0, has_side_effects=True, vmem_limit_bytes=64 * 1024 * 1024 - 65536 - 4096),
            name="decoder_block",
        )(jnp.transpose(features[0], (1, 2, 3, 0)), jnp.transpose(latent[0], (1, 3, 0, 2)), gn_gain, gn_bias, small(zy_weight), zy_bias,
          small(zb_weight), zb_bias, taps, conv_bias, up_taps, up_bias.reshape(1, n_chan))
        return jnp.transpose(result, (3, 0, 2, 1))[None]

    data_spec = P("dp", None, None, "sh", "sw")
    return jax.shard_map(local_step, mesh=mesh, in_specs=(data_spec, data_spec) + (P(),) * 10, out_specs=data_spec, check_vma=False)
```
